512 devices in a mesh: groups: 2 (over y), ffn: 16 (over x, core), width: 16 (over z).
Axes of the slice: x: 8, y: 2, z: 16, core: 2. Of those that a mesh axis runs over, the one named last changes fastest.
The devices are a block of a 8x8x16 slice.
Arguments:
- hidden: bfloat16 [2048, 8192], P(('groups', 'ffn'), 'width'), parts along dimension 0, may hold values from -8.4 to 8.4
- upstream: bfloat16 [2048, 8192], P(('groups', 'ffn'), 'width'), parts along dimension 0, may hold values from -6 to 6
- query_frozen_weight: bfloat16 [8192, 8192], P('width', 'ffn'), may hold values from -0.0625 to 0.0625
- key_value_frozen_weight: bfloat16 [2, 8192, 1024], P(None, 'width', 'ffn'), may hold values from -0.0625 to 0.0625
- output_frozen_weight: bfloat16 [8192, 8192], P('ffn', 'width'), may hold values from -0.0625 to 0.0625
- adapter_down: bfloat16 [6, 16, 8192], P('groups', None, 'width'), parts along dimension 0, may hold values from -0.0625 to 0.0625
- query_up_map: bfloat16 [32, 8192], P('groups', 'ffn'), parts along dimension 0, may hold values from -0.0625 to 0.0625
- key_value_up_maps: bfloat16 [4, 16, 1024], P('groups', None, 'ffn'), parts along dimension 0, may hold values from -0.0625 to 0.0625
- output_down_map: bfloat16 [32, 8192], P('groups', 'ffn'), parts along dimension 0, may hold values from -0.0625 to 0.0625
- output_up: bfloat16 [32, 8192], P('groups', 'width'), parts along dimension 0, may hold values from -0.0625 to 0.0625
Outputs:
- hidden_gradient: bfloat16 [2048, 8192], P(('groups', 'ffn'), 'width'), parts along dimension 0
- down_map_gradient: float32 [6, 16, 8192], P('groups', None, 'width'), parts along dimension 0
- query_up_map_gradient: float32 [32, 8192], P('groups', 'ffn'), parts along dimension 0
- key_value_up_maps_gradient: float32 [4, 16, 1024], P('groups', None, 'ffn'), parts along dimension 0
- output_down_map_gradient: float32 [32, 8192], P('groups', 'ffn'), parts along dimension 0
- output_up_map_gradient: float32 [32, 8192], P('groups', 'width'), parts along dimension 0
The draws below stay inside these ranges and needn't reach their ends.
There are 2 independent parts, one for each index of `groups`. The reference program is written for one: setup_inputs(seed, part) draws one part's arguments, and reference() takes and returns one part's arrays. A program takes and returns all parts, laid end to end along the dimension named above; an argument that names none is the same for every part. Nothing has to cross between parts.
All inputs are finite; a program needn't handle non-finite values.
Results may differ from the reference program's by a relative error of at most 0.04.
Values may be sent and summed in bfloat16 or wider, within the bound.
No kernel may reach another device: no remote copies, remote signals or barrier semaphores. Data moves between devices by JAX's collectives and lax.ppermute only.
A program may use at most 64 MiB of HBM per device.

```python
import math
import jax
import jax.numpy as jnp
from jax import lax

MODEL_WIDTH = 8192
HEADS = 64
KV_HEADS = 8
HEAD_DIM = 128
ADAPTER_RANK = 16
TOKENS = 1024
N_FFN = 16
N_WIDTH = 16


def draw_hidden(key, part):
    base_key = jax.random.fold_in(jax.random.fold_in(key, 11), 0)
    values = jnp.clip(jax.random.normal(base_key, (TOKENS, MODEL_WIDTH), jnp.float32), -6.0, 6.0)
    return values.astype(jnp.bfloat16)


def steps_of(rng, dims, cuts, smallest, top_value):
    level = 1.0
    for dim, blocks in cuts:
        draws = jax.random.uniform(jax.random.fold_in(jax.random.fold_in(rng, 6), dim), (blocks,), jnp.float32, smallest / len(cuts), top_value / len(cuts))
        level = level * jnp.repeat(jnp.exp(draws), dims[dim] // blocks).reshape((-1,) + (1,) * (len(dims) - 1 - dim))
    return level


def normal_values(own_key, dims, scale, bound, cuts=(), held_as=jnp.bfloat16):
    drawn = scale * jax.random.normal(own_key, dims, jnp.float32)
    if cuts:
        drawn = drawn * steps_of(own_key, dims, cuts, -0.22, 0.18)
    return jnp.clip(drawn, -bound, bound).astype(held_as)


def setup_inputs(seed: int = 0, part: int = 0) -> dict:
    splits = jax.random.split(jax.random.key(seed), 11)
    own_keys = jax.random.split(jax.random.fold_in(splits[10], part), 11)
    return {
        "hidden": draw_hidden(jax.random.fold_in(jax.random.fold_in(splits[10], part), 71), part),
        "upstream": normal_values(own_keys[1], (TOKENS, MODEL_WIDTH), 1.0, 6.0, ((0, 16), (1, 16))),
        "query_frozen_weight": normal_values(splits[2], (MODEL_WIDTH, HEADS * HEAD_DIM), MODEL_WIDTH ** -0.5, 0.0625, ((0, 16), (1, 16))),
        "key_value_frozen_weight": normal_values(splits[3], (2, MODEL_WIDTH, KV_HEADS * HEAD_DIM), MODEL_WIDTH ** -0.5, 0.0625, ((1, 16), (2, 16))),
        "output_frozen_weight": normal_values(splits[4], (HEADS * HEAD_DIM, MODEL_WIDTH), (HEADS * HEAD_DIM) ** -0.5, 0.0625, ((0, 16), (1, 16))),
        "adapter_down": normal_values(own_keys[5], (3, ADAPTER_RANK, MODEL_WIDTH), MODEL_WIDTH ** -0.5, 0.0625, ((2, 16),)),
        "query_up_map": normal_values(own_keys[6], (ADAPTER_RANK, HEADS * HEAD_DIM), MODEL_WIDTH ** -0.5, 0.0625, ((1, 16),)),
        "key_value_up_maps": normal_values(own_keys[7], (2, ADAPTER_RANK, KV_HEADS * HEAD_DIM), MODEL_WIDTH ** -0.5, 0.0625, ((2, 16),)),
        "output_down_map": normal_values(own_keys[8], (ADAPTER_RANK, HEADS * HEAD_DIM), (HEADS * HEAD_DIM) ** -0.5, 0.0625, ((1, 16),)),
        "output_up": normal_values(own_keys[9], (ADAPTER_RANK, MODEL_WIDTH), MODEL_WIDTH ** -0.5, 0.0625, ((1, 16),)),
    }


adapter_scale = 2.0
rope_base = 500000.0

def rotate(values, positions, first_dim, direction):
    columns = values.shape[1]
    head_dims = (first_dim + jnp.arange(columns, dtype=jnp.int32)) % HEAD_DIM
    pair_dims = head_dims - head_dims % 2
    frequency = jnp.exp(pair_dims.astype(jnp.float32) * (-math.log(rope_base) / HEAD_DIM))
    angles = positions.astype(jnp.float32)[:, None] * frequency[None, :]
    is_even = head_dims % 2 == 0
    following = jnp.roll(values, -1, axis=1)
    preceding = jnp.roll(values, 1, axis=1)
    partner = jnp.where(is_even[None, :], -following, preceding)
    return values * jnp.cos(angles) + direction * partner * jnp.sin(angles)

def width_grouped(left_side, right_side):
    block_size = left_side.shape[1] // N_WIDTH
    running = jnp.zeros((left_side.shape[0], right_side.shape[1]), jnp.float32)
    for block_index in range(N_WIDTH):
        offset = block_index * block_size
        partial_value = jnp.dot(left_side[:, offset:offset + block_size], right_side[offset:offset + block_size, :], preferred_element_type=jnp.float32)
        running = running + lax.optimization_barrier(partial_value.astype(jnp.bfloat16)).astype(jnp.float32)
    return running

def head_grouped(contraction_pairs, token_count):
    running = jnp.zeros((token_count, MODEL_WIDTH), jnp.float32)
    for block_index in range(N_FFN):
        partial_value = jnp.zeros((token_count, MODEL_WIDTH), jnp.float32)
        for gradient, weight in contraction_pairs:
            block_size = weight.shape[1] // N_FFN
            offset = block_index * block_size
            partial_value = partial_value + jnp.dot(gradient[:, offset:offset + block_size], weight[:, offset:offset + block_size].T, preferred_element_type=jnp.float32)
        running = running + lax.optimization_barrier(partial_value.astype(jnp.bfloat16)).astype(jnp.float32)
    return running

def reference(hidden, upstream, query_frozen_weight, key_value_frozen_weight, output_frozen_weight, adapter_down, query_up_map, key_value_up_maps, output_down_map, output_up):
    token_count = hidden.shape[0]
    group_size = HEADS // KV_HEADS
    score_scale = 1.0 / math.sqrt(HEAD_DIM)
    positions = jnp.arange(token_count, dtype=jnp.int32)
    down_flattened = adapter_down.reshape(3 * ADAPTER_RANK, MODEL_WIDTH)
    reduced_hidden = jnp.dot(hidden, down_flattened.T, preferred_element_type=jnp.float32).astype(jnp.bfloat16)
    reduced_query = reduced_hidden[:, :ADAPTER_RANK]
    reduced_key = reduced_hidden[:, ADAPTER_RANK:2 * ADAPTER_RANK]
    reduced_value = reduced_hidden[:, 2 * ADAPTER_RANK:]
    output_reduced = jnp.dot(upstream, output_up.T, preferred_element_type=jnp.float32).astype(jnp.bfloat16)
    query_projected = width_grouped(hidden, query_frozen_weight) + adapter_scale * jnp.dot(reduced_query, query_up_map, preferred_element_type=jnp.float32)
    query_states = rotate(query_projected, positions, 0, 1.0).astype(jnp.bfloat16)
    key_projected = width_grouped(hidden, key_value_frozen_weight[0]) + adapter_scale * jnp.dot(reduced_key, key_value_up_maps[0], preferred_element_type=jnp.float32)
    key_states = rotate(key_projected, positions, 0, 1.0).astype(jnp.bfloat16)
    value_state_rows = (width_grouped(hidden, key_value_frozen_weight[1]) + adapter_scale * jnp.dot(reduced_value, key_value_up_maps[1], preferred_element_type=jnp.float32)).astype(jnp.bfloat16)
    attention_output_gradient = (width_grouped(upstream, output_frozen_weight.T) + adapter_scale * jnp.dot(output_reduced, output_down_map, preferred_element_type=jnp.float32)).astype(jnp.bfloat16)
    query_heads = query_states.reshape(token_count, KV_HEADS, group_size, HEAD_DIM).transpose(1, 0, 2, 3)
    grad_heads = attention_output_gradient.reshape(token_count, KV_HEADS, group_size, HEAD_DIM).transpose(1, 0, 2, 3)
    key_heads = key_states.reshape(token_count, KV_HEADS, HEAD_DIM).transpose(1, 0, 2)
    value_heads = value_state_rows.reshape(token_count, KV_HEADS, HEAD_DIM).transpose(1, 0, 2)
    causal = positions[:, None] >= positions[None, :]

    def one_head(head_items):
        query_one = head_items[0].astype(jnp.float32)
        key_one = head_items[1].astype(jnp.float32)
        value_one = head_items[2].astype(jnp.float32)
        grad_one = head_items[3].astype(jnp.float32)
        scores = jnp.einsum('tgd,sd->gts', query_one, key_one) * score_scale
        scores = jnp.where(causal[None, :, :], scores, -jnp.inf)
        shifted = jnp.exp(scores - lax.optimization_barrier(jnp.max(scores, axis=-1, keepdims=True)))
        probs = shifted / lax.optimization_barrier(jnp.sum(shifted, axis=-1, keepdims=True))
        prob_weights = lax.optimization_barrier(probs.astype(jnp.bfloat16)).astype(jnp.float32)
        attention_one = jnp.einsum('gts,sd->tgd', prob_weights, value_one).astype(jnp.bfloat16)
        prob_grad = jnp.einsum('tgd,sd->gts', grad_one, value_one)
        delta = jnp.einsum('tgd,tgd->gt', grad_one, attention_one.astype(jnp.float32))
        score_grad = lax.optimization_barrier((probs * (prob_grad - delta[:, :, None]) * score_scale).astype(jnp.bfloat16)).astype(jnp.float32)
        query_rot = jnp.einsum('gts,sd->tgd', score_grad, key_one)
        key_rot = jnp.einsum('gts,tgd->sd', score_grad, query_one)
        value_grad = jnp.einsum('gts,tgd->sd', prob_weights, grad_one)
        return (attention_one, query_rot, key_rot, value_grad)
    attention_heads, query_rots, key_rots, value_grads = lax.map(one_head, (query_heads, key_heads, value_heads, grad_heads))
    attention_output = attention_heads.transpose(1, 0, 2, 3).reshape(token_count, HEADS * HEAD_DIM)
    query_rot_all = query_rots.transpose(1, 0, 2, 3).reshape(token_count, HEADS * HEAD_DIM)
    key_rot_all = key_rots.transpose(1, 0, 2).reshape(token_count, KV_HEADS * HEAD_DIM)
    value_all = value_grads.transpose(1, 0, 2).reshape(token_count, KV_HEADS * HEAD_DIM)
    query_rows_gradient = rotate(query_rot_all, positions, 0, -1.0).astype(jnp.bfloat16)
    key_rows_gradient = rotate(key_rot_all, positions, 0, -1.0).astype(jnp.bfloat16)
    value_rows_gradient = value_all.astype(jnp.bfloat16)
    rank_gradient = jnp.concatenate([jnp.dot(query_rows_gradient, query_up_map.T, preferred_element_type=jnp.float32), jnp.dot(key_rows_gradient, key_value_up_maps[0].T, preferred_element_type=jnp.float32), jnp.dot(value_rows_gradient, key_value_up_maps[1].T, preferred_element_type=jnp.float32)], axis=1).astype(jnp.bfloat16)
    contraction_pairs = ((query_rows_gradient, query_frozen_weight), (key_rows_gradient, key_value_frozen_weight[0]), (value_rows_gradient, key_value_frozen_weight[1]))
    hidden_gradient_total = head_grouped(contraction_pairs, token_count) + adapter_scale * jnp.dot(rank_gradient, down_flattened, preferred_element_type=jnp.float32)
    hidden_gradient = hidden_gradient_total.astype(jnp.bfloat16)
    down_map_gradient = (adapter_scale * jnp.dot(rank_gradient.T, hidden, preferred_element_type=jnp.float32)).reshape(3, ADAPTER_RANK, MODEL_WIDTH)
    query_up_map_gradient = adapter_scale * jnp.dot(reduced_query.T, query_rows_gradient, preferred_element_type=jnp.float32)
    key_value_up_maps_gradient = adapter_scale * jnp.stack([jnp.dot(reduced_key.T, key_rows_gradient, preferred_element_type=jnp.float32), jnp.dot(reduced_value.T, value_rows_gradient, preferred_element_type=jnp.float32)])
    outer_product_rank = jnp.dot(attention_output, output_down_map.T, preferred_element_type=jnp.float32).astype(jnp.bfloat16)
    output_down_map_gradient = adapter_scale * jnp.dot(output_reduced.T, attention_output, preferred_element_type=jnp.float32)
    output_up_map_gradient = adapter_scale * jnp.dot(outer_product_rank.T, upstream, preferred_element_type=jnp.float32)
    return (hidden_gradient, down_map_gradient, query_up_map_gradient, key_value_up_maps_gradient, output_down_map_gradient, output_up_map_gradient)
```

```python
import math

import jax
import jax.numpy as jnp
from jax import lax
from jax.sharding import PartitionSpec as P

HEAD_DIM = 128
ADAPTER_RANK = 16

adapter_scale = 2.0
rope_base = 500000.0

f32 = jnp.float32
bf16 = jnp.bfloat16


def dot(a, b):
    return jnp.dot(a, b, preferred_element_type=f32)


def dot_nt(a, b):
    return lax.dot_general(a, b, (((1,), (1,)), ((), ())), preferred_element_type=f32)


def dot_tn(a, b):
    return lax.dot_general(a, b, (((0,), (0,)), ((), ())), preferred_element_type=f32)


def by_core(size):
    return [[2 * k + c for k in range(size // 2)] for c in range(2)]


def from_partner(array):
    return lax.ppermute(array, "ffn", [(i, i ^ 1) for i in range(lax.axis_size("ffn"))])


def sent_to_all(array, axis, groups=None):
    size = len(groups[0]) if groups else lax.axis_size(axis)
    copies = jnp.broadcast_to(array[None], (size, *array.shape))
    return lax.all_to_all(copies, axis, 0, 0, tiled=True, axis_index_groups=groups)


def pieces_summed(array, axis, groups=None):
    size = len(groups[0]) if groups else lax.axis_size(axis)
    pieces = array.reshape(size, array.shape[0] // size, *array.shape[1:])
    arrived = lax.all_to_all(pieces, axis, 0, 0, tiled=True, axis_index_groups=groups)
    return arrived.astype(f32).sum(axis=0)


def rope_tables(positions, first_dim, columns):
    dims = (first_dim + jnp.arange(columns, dtype=jnp.int32)) % HEAD_DIM
    pair_dims = dims - dims % 2
    frequency = jnp.exp(pair_dims.astype(f32) * (-math.log(rope_base) / HEAD_DIM))
    angles = positions.astype(f32)[:, None] * frequency[None, :]
    return jnp.cos(angles), jnp.sin(angles)


def rotate(values, tables, direction):
    cos, sin = tables
    is_even = jnp.arange(values.shape[-1], dtype=jnp.int32) % 2 == 0
    following = jnp.roll(values, -1, axis=-1)
    preceding = jnp.roll(values, 1, axis=-1)
    partner = jnp.where(is_even, -following, preceding)
    return values * cos + direction * partner * sin


def shards(
    hidden,
    upstream,
    query_frozen_weight,
    key_value_frozen_weight,
    output_frozen_weight,
    adapter_down,
    query_up_map,
    key_value_up_maps,
    output_down_map,
    output_up,
):
    ffn_count = lax.axis_size("ffn")
    width_count = lax.axis_size("width")
    ffn_index = lax.axis_index("ffn")
    width_index = lax.axis_index("width")
    parity = ffn_index % 2
    same_core = by_core(ffn_count)
    own_rows, width_cols = hidden.shape
    token_count = own_rows * ffn_count
    query_rows = token_count // width_count
    query_cols = query_frozen_weight.shape[1]
    key_cols = key_value_frozen_weight.shape[2]
    heads = query_cols // HEAD_DIM
    rank = ADAPTER_RANK
    score_scale = 1.0 / math.sqrt(HEAD_DIM)
    row_positions = width_index * query_rows + jnp.arange(query_rows, dtype=jnp.int32)

    query_weight = (
        query_frozen_weight.astype(f32) + adapter_scale * dot_tn(adapter_down[0], query_up_map)
    ).astype(bf16)
    key_value_weight = jnp.concatenate(
        [
            key_value_frozen_weight[k].astype(f32)
            + adapter_scale * dot_tn(adapter_down[k + 1], key_value_up_maps[k])
            for k in range(2)
        ],
        axis=1,
    ).astype(bf16)
    output_weight = (
        output_frozen_weight.astype(f32) + adapter_scale * dot_tn(output_down_map, output_up)
    ).astype(bf16)
    down = adapter_down.reshape(3 * rank, width_cols)
    from_hidden = jnp.concatenate(
        [query_weight, jnp.zeros((width_cols, query_cols), bf16), down.T], axis=1
    )
    from_upstream = jnp.concatenate(
        [jnp.zeros((width_cols, query_cols), bf16), output_weight.T], axis=1
    )
    pad = 128
    from_hidden = jnp.pad(from_hidden, ((0, 0), (0, pad - 3 * rank)))
    from_upstream = jnp.concatenate(
        [
            from_upstream,
            jnp.zeros((width_cols, 3 * rank), bf16),
            output_up.T,
            jnp.zeros((width_cols, pad - 4 * rank), bf16),
        ],
        axis=1,
    )
    joint_weight = jnp.concatenate([from_hidden, from_upstream], axis=0)
    query_tables = rope_tables(row_positions, 0, HEAD_DIM)
    key_tables = rope_tables(row_positions, ffn_index * key_cols, key_cols)
    joint_weight, key_value_weight, query_weight, query_tables, key_tables = (
        lax.optimization_barrier(
            (joint_weight, key_value_weight, query_weight, query_tables, key_tables)
        )
    )

    both = jnp.concatenate([hidden, upstream], axis=1)
    own_core = sent_to_all(both, "ffn", same_core)
    other_core = from_partner(own_core)
    rows = jnp.where(
        parity == 0,
        jnp.stack([own_core, other_core], axis=1),
        jnp.stack([other_core, own_core], axis=1),
    ).reshape(token_count, 2 * width_cols)
    hidden_rows = rows[:, :width_cols]
    upstream_rows = rows[:, width_cols:]

    joint_part = dot(rows, joint_weight).astype(bf16)
    joint_rows = lax.psum_scatter(joint_part, "width", scatter_dimension=0, tiled=True)

    key_value_part = dot(hidden_rows, key_value_weight).astype(bf16)
    key_value_sum = pieces_summed(key_value_part, "width")
    key_value_rows = jnp.concatenate(
        [rotate(key_value_sum[:, :key_cols], key_tables, 1.0), key_value_sum[:, key_cols:]], axis=1
    ).astype(bf16)
    own_half = sent_to_all(key_value_rows, "width").reshape(token_count, 2 * key_cols)
    other_half = from_partner(own_half)
    first = jnp.where(parity == 0, own_half, other_half)
    second = jnp.where(parity == 0, other_half, own_half)
    key_states = jnp.concatenate([first[:, :key_cols], second[:, :key_cols]], axis=1)
    value_states = jnp.concatenate([first[:, key_cols:], second[:, key_cols:]], axis=1)

    def by_head(values):
        return values.reshape(query_rows, heads, HEAD_DIM).transpose(1, 0, 2)

    def by_row(values):
        return (
            values.reshape(heads, query_rows, HEAD_DIM)
            .transpose(1, 0, 2)
            .reshape(query_rows, query_cols)
        )

    low_rows = joint_rows[:, 2 * query_cols : 2 * query_cols + 4 * rank]
    query = (
        rotate(by_head(joint_rows[:, :query_cols].astype(f32)), query_tables, 1.0)
        .astype(bf16)
        .reshape(heads * query_rows, HEAD_DIM)
    )
    grad = by_head(joint_rows[:, query_cols : 2 * query_cols]).reshape(
        heads * query_rows, HEAD_DIM
    )
    positions = jnp.arange(token_count, dtype=jnp.int32)
    causal = jnp.tile(row_positions, heads)[:, None] >= positions[None, :]
    scores = jnp.where(causal, dot_nt(query, key_states) * score_scale, -jnp.inf)
    shifted = jnp.exp(scores - jnp.max(scores, axis=-1, keepdims=True))
    probs = shifted / jnp.sum(shifted, axis=-1, keepdims=True)
    prob_weights = probs.astype(bf16)
    attention = dot(prob_weights, value_states).astype(bf16)
    prob_grad = dot_nt(grad, value_states)
    delta = jnp.sum(grad.astype(f32) * attention.astype(f32), axis=-1, keepdims=True)
    score_grad = (probs * (prob_grad - delta) * score_scale).astype(bf16)
    query_grad = by_row(
        rotate(
            dot(score_grad, key_states).reshape(heads, query_rows, HEAD_DIM), query_tables, -1.0
        ).astype(bf16)
    )
    key_part_grad = dot_tn(score_grad, query)
    value_part_grad = dot_tn(prob_weights, grad)
    attention_rows = by_row(attention)

    output_down_part = dot_tn(low_rows[:, 3 * rank :], attention_rows).astype(bf16)
    riding = jnp.concatenate(
        [query_grad, output_down_part.reshape(query_rows, -1), low_rows], axis=1
    )
    gathered = lax.all_gather(riding, "width", axis=0, tiled=True)

    def halves(own):
        start = jnp.where(own, parity, 1 - parity) * key_cols
        return jnp.concatenate(
            [
                lax.dynamic_slice_in_dim(key_part_grad, start, key_cols, 1),
                lax.dynamic_slice_in_dim(value_part_grad, start, key_cols, 1),
            ],
            axis=1,
        )

    received = from_partner(halves(False).astype(bf16))
    key_value_total = (halves(True) + received.astype(f32)).astype(bf16)
    key_value_grad_sum = pieces_summed(key_value_total, "width")
    key_grad = rotate(key_value_grad_sum[:, :key_cols], key_tables, -1.0).astype(bf16)
    value_grad = key_value_grad_sum[:, key_cols:].astype(bf16)
    terms = jnp.concatenate(
        [
            dot_nt(query_grad, query_up_map),
            dot_nt(key_grad, key_value_up_maps[0]),
            dot_nt(value_grad, key_value_up_maps[1]),
            dot_nt(attention_rows, output_down_map),
        ],
        axis=1,
    )
    terms = terms + from_partner(terms)
    terms = sent_to_all(terms, "ffn", same_core).sum(axis=0).astype(bf16)
    key_value_riding = jnp.concatenate([key_grad, value_grad, terms], axis=1)
    key_value_gathered = sent_to_all(key_value_riding, "width").reshape(token_count, -1)

    query_grad_rows = gathered[:, :query_cols]
    key_value_grad_rows = key_value_gathered[:, : 2 * key_cols]

    input_part = dot_nt(query_grad_rows, query_weight) + dot_nt(
        key_value_grad_rows, key_value_weight
    )
    by_owner = input_part.reshape(ffn_count // 2, 2, own_rows, width_cols)
    kept = lax.dynamic_index_in_dim(by_owner, parity, 1, keepdims=False)
    given = lax.dynamic_index_in_dim(by_owner, 1 - parity, 1, keepdims=False).astype(bf16)
    pair_sum = (kept + from_partner(given).astype(f32)).astype(bf16)
    hidden_gradient = pieces_summed(
        pair_sum.reshape(ffn_count // 2 * own_rows, width_cols), "ffn", same_core
    ).astype(bf16)

    low = gathered[:, query_cols + 2 * key_cols :]
    rank_gradient = key_value_gathered[:, 2 * key_cols : 2 * key_cols + 3 * rank]
    outer_rank = key_value_gathered[:, 2 * key_cols + 3 * rank :]
    down_map_gradient = (adapter_scale * dot_tn(rank_gradient, hidden_rows)).reshape(
        adapter_down.shape
    )
    query_up_map_gradient = adapter_scale * dot_tn(low[:, :rank], query_grad_rows)
    key_value_up_maps_gradient = adapter_scale * jnp.stack(
        [
            dot_tn(low[:, rank : 2 * rank], key_value_grad_rows[:, :key_cols]),
            dot_tn(low[:, 2 * rank : 3 * rank], key_value_grad_rows[:, key_cols:]),
        ]
    )
    output_down_map_gradient = adapter_scale * gathered[
        :, query_cols : query_cols + 2 * key_cols
    ].reshape(width_count, query_rows, 2 * key_cols).astype(f32).sum(axis=0).reshape(
        rank, query_cols
    )
    output_up_map_gradient = adapter_scale * dot_tn(outer_rank, upstream_rows)
    return (
        hidden_gradient,
        down_map_gradient,
        query_up_map_gradient,
        key_value_up_maps_gradient,
        output_down_map_gradient,
        output_up_map_gradient,
    )


def solution(mesh):
    placed = (
        P(("groups", "ffn"), "width"),
        P(("groups", "ffn"), "width"),
        P("width", "ffn"),
        P(None, "width", "ffn"),
        P("ffn", "width"),
        P("groups", None, "width"),
        P("groups", "ffn"),
        P("groups", None, "ffn"),
        P("groups", "ffn"),
        P("groups", "width"),
    )
    return jax.shard_map(
        shards,
        mesh=mesh,
        in_specs=placed,
        out_specs=(
            P(("groups", "ffn"), "width"),
            P("groups", None, "width"),
            P("groups", "ffn"),
            P("groups", None, "ffn"),
            P("groups", "ffn"),
            P("groups", "width"),
        ),
        check_vma=False,
    )
```

```python
import math

import jax
import jax.numpy as jnp
from jax import lax
from jax.sharding import PartitionSpec as P


HEAD_DIM = 128
ADAPTER_RANK = 16

adapter_scale = 2.0
rope_base = 500000.0

f32 = jnp.float32
bf16 = jnp.bfloat16


def dot(a, b):
    return jnp.dot(a, b, preferred_element_type=f32)


def dot_nt(a, b):
    return lax.dot_general(a, b, (((1,), (1,)), ((), ())), preferred_element_type=f32)


def dot_tn(a, b):
    return lax.dot_general(a, b, (((0,), (0,)), ((), ())), preferred_element_type=f32)


def by_core(size):
    return [[2 * k + c for k in range(size // 2)] for c in range(2)]


def from_partner(array):
    return lax.ppermute(array, "ffn", [(i, i ^ 1) for i in range(lax.axis_size("ffn"))])


def sent_to_all(array, axis, groups=None):
    size = len(groups[0]) if groups else lax.axis_size(axis)
    copies = jnp.broadcast_to(array[None], (size, *array.shape))
    return lax.all_to_all(copies, axis, 0, 0, tiled=True, axis_index_groups=groups)


def pieces_summed(array, axis, groups=None):
    size = len(groups[0]) if groups else lax.axis_size(axis)
    pieces = array.reshape(size, array.shape[0] // size, *array.shape[1:])
    arrived = lax.all_to_all(pieces, axis, 0, 0, tiled=True, axis_index_groups=groups)
    return arrived.astype(f32).sum(axis=0)


def rope_tables(positions, first_dim, columns):
    dims = (first_dim + jnp.arange(columns, dtype=jnp.int32)) % HEAD_DIM
    pair_dims = dims - dims % 2
    frequency = jnp.exp(pair_dims.astype(f32) * (-math.log(rope_base) / HEAD_DIM))
    angles = positions.astype(f32)[:, None] * frequency[None, :]
    return jnp.cos(angles), jnp.sin(angles)


def rotate(values, tables, direction):
    cos, sin = tables
    is_even = jnp.arange(values.shape[-1], dtype=jnp.int32) % 2 == 0
    following = jnp.roll(values, -1, axis=-1)
    preceding = jnp.roll(values, 1, axis=-1)
    partner = jnp.where(is_even, -following, preceding)
    return values * cos + direction * partner * sin


def shards(
    hidden,
    upstream,
    query_frozen_weight,
    key_value_frozen_weight,
    output_frozen_weight,
    adapter_down,
    query_up_map,
    key_value_up_maps,
    output_down_map,
    output_up,
):
    ffn_count = lax.axis_size("ffn")
    width_count = lax.axis_size("width")
    ffn_index = lax.axis_index("ffn")
    width_index = lax.axis_index("width")
    parity = ffn_index % 2
    same_core = by_core(ffn_count)
    own_rows, width_cols = hidden.shape
    token_count = own_rows * ffn_count
    query_rows = token_count // width_count
    query_cols = query_frozen_weight.shape[1]
    key_cols = key_value_frozen_weight.shape[2]
    heads = query_cols // HEAD_DIM
    rank = ADAPTER_RANK
    score_scale = 1.0 / math.sqrt(HEAD_DIM)
    row_positions = width_index * query_rows + jnp.arange(query_rows, dtype=jnp.int32)

    query_weight = (
        query_frozen_weight.astype(f32) + adapter_scale * dot_tn(adapter_down[0], query_up_map)
    ).astype(bf16)
    key_value_weight = jnp.concatenate(
        [
            key_value_frozen_weight[k].astype(f32)
            + adapter_scale * dot_tn(adapter_down[k + 1], key_value_up_maps[k])
            for k in range(2)
        ],
        axis=1,
    ).astype(bf16)
    output_weight = (
        output_frozen_weight.astype(f32) + adapter_scale * dot_tn(output_down_map, output_up)
    ).astype(bf16)
    down = adapter_down.reshape(3 * rank, width_cols)
    from_hidden = jnp.concatenate(
        [query_weight, jnp.zeros((width_cols, query_cols), bf16), down.T], axis=1
    )
    from_upstream = jnp.concatenate(
        [jnp.zeros((width_cols, query_cols), bf16), output_weight.T], axis=1
    )
    pad = 128
    from_hidden = jnp.pad(from_hidden, ((0, 0), (0, pad - 3 * rank)))
    from_upstream = jnp.concatenate(
        [
            from_upstream,
            jnp.zeros((width_cols, 3 * rank), bf16),
            output_up.T,
            jnp.zeros((width_cols, pad - 4 * rank), bf16),
        ],
        axis=1,
    )
    joint_weight = jnp.concatenate([from_hidden, from_upstream], axis=0)
    query_tables = rope_tables(row_positions, 0, HEAD_DIM)
    key_tables = rope_tables(row_positions, ffn_index * key_cols, key_cols)
    joint_weight, key_value_weight, query_weight, query_tables, key_tables = (
        lax.optimization_barrier(
            (joint_weight, key_value_weight, query_weight, query_tables, key_tables)
        )
    )

    both = jnp.concatenate([hidden, upstream], axis=1)
    own_core = sent_to_all(both, "ffn", same_core)
    other_core = from_partner(own_core)
    rows = jnp.where(
        parity == 0,
        jnp.stack([own_core, other_core], axis=1),
        jnp.stack([other_core, own_core], axis=1),
    ).reshape(token_count, 2 * width_cols)
    hidden_rows = rows[:, :width_cols]
    upstream_rows = rows[:, width_cols:]

    joint_part = dot(rows, joint_weight).astype(bf16)
    joint_rows = lax.psum_scatter(joint_part, "width", scatter_dimension=0, tiled=True)

    key_value_part = dot(hidden_rows, key_value_weight).astype(bf16)
    key_value_sum = pieces_summed(key_value_part, "width")
    key_value_rows = jnp.concatenate(
        [rotate(key_value_sum[:, :key_cols], key_tables, 1.0), key_value_sum[:, key_cols:]], axis=1
    ).astype(bf16)
    own_half = lax.all_gather(key_value_rows, "width", axis=0, tiled=True)
    other_half = from_partner(own_half)
    first = jnp.where(parity == 0, own_half, other_half)
    second = jnp.where(parity == 0, other_half, own_half)
    key_states = jnp.concatenate([first[:, :key_cols], second[:, :key_cols]], axis=1)
    value_states = jnp.concatenate([first[:, key_cols:], second[:, key_cols:]], axis=1)

    def by_head(values):
        return values.reshape(query_rows, heads, HEAD_DIM).transpose(1, 0, 2)

    def by_row(values):
        return (
            values.reshape(heads, query_rows, HEAD_DIM)
            .transpose(1, 0, 2)
            .reshape(query_rows, query_cols)
        )

    low_rows = joint_rows[:, 2 * query_cols : 2 * query_cols + 4 * rank]
    query = (
        rotate(by_head(joint_rows[:, :query_cols].astype(f32)), query_tables, 1.0)
        .astype(bf16)
        .reshape(heads * query_rows, HEAD_DIM)
    )
    grad = by_head(joint_rows[:, query_cols : 2 * query_cols]).reshape(
        heads * query_rows, HEAD_DIM
    )
    positions = jnp.arange(token_count, dtype=jnp.int32)
    causal = jnp.tile(row_positions, heads)[:, None] >= positions[None, :]
    scores = jnp.where(causal, dot_nt(query, key_states) * score_scale, -jnp.inf)
    shifted = jnp.exp(scores - jnp.max(scores, axis=-1, keepdims=True))
    probs = shifted / jnp.sum(shifted, axis=-1, keepdims=True)
    prob_weights = probs.astype(bf16)
    attention = dot(prob_weights, value_states).astype(bf16)
    prob_grad = dot_nt(grad, value_states)
    delta = jnp.sum(grad.astype(f32) * attention.astype(f32), axis=-1, keepdims=True)
    score_grad = (probs * (prob_grad - delta) * score_scale).astype(bf16)
    query_grad = by_row(
        rotate(
            dot(score_grad, key_states).reshape(heads, query_rows, HEAD_DIM), query_tables, -1.0
        ).astype(bf16)
    )
    key_part_grad = dot_tn(score_grad, query)
    value_part_grad = dot_tn(prob_weights, grad)
    attention_rows = by_row(attention)

    output_down_part = dot_tn(low_rows[:, 3 * rank :], attention_rows).astype(bf16)
    riding = jnp.concatenate(
        [query_grad, output_down_part.reshape(query_rows, -1), low_rows], axis=1
    )
    riding, key_part_grad, value_part_grad, query_grad, attention_rows = lax.optimization_barrier(
        (riding, key_part_grad, value_part_grad, query_grad, attention_rows)
    )
    gathered = lax.all_gather(riding, "width", axis=0, tiled=True)

    def halves(own):
        start = jnp.where(own, parity, 1 - parity) * key_cols
        return jnp.concatenate(
            [
                lax.dynamic_slice_in_dim(key_part_grad, start, key_cols, 1),
                lax.dynamic_slice_in_dim(value_part_grad, start, key_cols, 1),
            ],
            axis=1,
        )

    received = from_partner(halves(False).astype(bf16))
    key_value_total = (halves(True) + received.astype(f32)).astype(bf16)
    key_value_grad_sum = pieces_summed(key_value_total, "width")
    key_value_grad = jnp.concatenate(
        [
            rotate(key_value_grad_sum[:, :key_cols], key_tables, -1.0),
            key_value_grad_sum[:, key_cols:],
        ],
        axis=1,
    ).astype(bf16)
    terms = jnp.concatenate(
        [
            dot_nt(query_grad, query_up_map),
            dot_nt(key_value_grad[:, :key_cols], key_value_up_maps[0]),
            dot_nt(key_value_grad[:, key_cols:], key_value_up_maps[1]),
            dot_nt(attention_rows, output_down_map),
        ],
        axis=1,
    ).astype(bf16)
    terms = sent_to_all(terms, "ffn").astype(f32).sum(axis=0).astype(bf16)
    key_value_gathered = lax.all_gather(
        jnp.concatenate([key_value_grad, terms], axis=1), "width", axis=0, tiled=True
    )
    key_value_grad_rows = key_value_gathered[:, : 2 * key_cols]

    input_weight = jnp.concatenate([query_weight, key_value_weight], axis=1)

    def input_part(of_core):
        def rows_of(values):
            by_owner = values.reshape(ffn_count // 2, 2, own_rows, -1)
            return lax.dynamic_index_in_dim(by_owner, of_core, 1, keepdims=False)

        grads = jnp.concatenate(
            [rows_of(gathered)[..., :query_cols], rows_of(key_value_grad_rows)], axis=-1
        ).reshape(ffn_count // 2 * own_rows, -1)
        return dot_nt(grads, input_weight)

    given = from_partner(input_part(1 - parity).astype(bf16))
    pair_sum = (input_part(parity) + given.astype(f32)).astype(bf16)
    hidden_gradient = pieces_summed(pair_sum, "ffn", same_core).astype(bf16)

    low = gathered[:, query_cols + 2 * key_cols :]
    rank_gradient = key_value_gathered[:, 2 * key_cols : 2 * key_cols + 3 * rank]
    outer_rank = key_value_gathered[:, 2 * key_cols + 3 * rank :]
    down_map_gradient = (adapter_scale * dot_tn(rank_gradient, hidden_rows)).reshape(
        adapter_down.shape
    )
    query_up_map_gradient = adapter_scale * dot_tn(low[:, :rank], gathered[:, :query_cols])
    key_value_up_maps_gradient = adapter_scale * jnp.stack(
        [
            dot_tn(low[:, rank : 2 * rank], key_value_grad_rows[:, :key_cols]),
            dot_tn(low[:, 2 * rank : 3 * rank], key_value_grad_rows[:, key_cols:]),
        ]
    )
    output_down_map_gradient = adapter_scale * gathered[
        :, query_cols : query_cols + 2 * key_cols
    ].reshape(width_count, query_rows, 2 * key_cols).astype(f32).sum(axis=0).reshape(
        rank, query_cols
    )
    output_up_map_gradient = adapter_scale * dot_tn(outer_rank, upstream_rows)
    return (
        hidden_gradient,
        down_map_gradient,
        query_up_map_gradient,
        key_value_up_maps_gradient,
        output_down_map_gradient,
        output_up_map_gradient,
    )


def solution(mesh):
    placed = (
        P(("groups", "ffn"), "width"),
        P(("groups", "ffn"), "width"),
        P("width", "ffn"),
        P(None, "width", "ffn"),
        P("ffn", "width"),
        P("groups", None, "width"),
        P("groups", "ffn"),
        P("groups", None, "ffn"),
        P("groups", "ffn"),
        P("groups", "width"),
    )
    return jax.shard_map(
        shards,
        mesh=mesh,
        in_specs=placed,
        out_specs=(
            P(("groups", "ffn"), "width"),
            P("groups", None, "width"),
            P("groups", "ffn"),
            P("groups", None, "ffn"),
            P("groups", "ffn"),
            P("groups", "width"),
        ),
        check_vma=False,
    )
```

```python
import functools
import math

import jax
import jax.numpy as jnp
from jax import lax
from jax.experimental import pallas as pl
from jax.experimental.pallas import tpu as pltpu
from jax.sharding import PartitionSpec as P


HEAD_DIM = 128
ADAPTER_RANK = 16

adapter_scale = 2.0
rope_base = 500000.0

f32 = jnp.float32
bf16 = jnp.bfloat16


def dot(a, b):
    return jnp.dot(a, b, preferred_element_type=f32)


def dot_nt(a, b):
    return lax.dot_general(a, b, (((1,), (1,)), ((), ())), preferred_element_type=f32)


def dot_tn(a, b):
    return lax.dot_general(a, b, (((0,), (0,)), ((), ())), preferred_element_type=f32)


def by_core(size):
    return [[2 * k + c for k in range(size // 2)] for c in range(2)]


def from_partner(array):
    return lax.ppermute(array, "ffn", [(i, i ^ 1) for i in range(lax.axis_size("ffn"))])


def sent_to_all(array, axis, groups=None):
    size = len(groups[0]) if groups else lax.axis_size(axis)
    copies = jnp.broadcast_to(array[None], (size, *array.shape))
    return lax.all_to_all(copies, axis, 0, 0, tiled=True, axis_index_groups=groups)


def pieces_summed(array, axis, groups=None):
    size = len(groups[0]) if groups else lax.axis_size(axis)
    pieces = array.reshape(size, array.shape[0] // size, *array.shape[1:])
    arrived = lax.all_to_all(pieces, axis, 0, 0, tiled=True, axis_index_groups=groups)
    return arrived.astype(f32).sum(axis=0)


def rope_tables(positions, first_dim, columns):
    dims = (first_dim + jnp.arange(columns, dtype=jnp.int32)) % HEAD_DIM
    pair_dims = dims - dims % 2
    frequency = jnp.exp(pair_dims.astype(f32) * (-math.log(rope_base) / HEAD_DIM))
    angles = positions.astype(f32)[:, None] * frequency[None, :]
    return jnp.cos(angles), jnp.sin(angles)


def rotate(values, tables, direction):
    cos, sin = tables
    is_even = jnp.arange(values.shape[-1], dtype=jnp.int32) % 2 == 0
    following = jnp.roll(values, -1, axis=-1)
    preceding = jnp.roll(values, 1, axis=-1)
    partner = jnp.where(is_even, -following, preceding)
    return values * cos + direction * partner * sin


def attention_block(
    place, joint, own, other, cos, sin, riding, attention_rows, kept, given, *, heads, scale
):
    swapped = place[0] == 1
    rows = joint.shape[0]
    cols = heads * HEAD_DIM
    half = HEAD_DIM // 2

    def stacked(start):
        return jnp.concatenate(
            [joint[:, start + h * HEAD_DIM : start + (h + 1) * HEAD_DIM] for h in range(heads)],
            axis=0,
        ).astype(f32)

    def turned(values):
        return pltpu.roll(values, half, 1)

    def reordered(values):
        return jnp.where(swapped, turned(values), values)

    lane = lax.broadcasted_iota(jnp.int32, (heads * rows, HEAD_DIM), 1)
    first_half = lane < half
    is_even = lane % 2 == 0
    cosines = jnp.concatenate([cos[...]] * heads, axis=0)
    sines = jnp.concatenate([sin[...]] * heads, axis=0)

    def rope(values, direction):
        partner = jnp.where(
            is_even, -pltpu.roll(values, HEAD_DIM - 1, 1), pltpu.roll(values, 1, 1)
        )
        return values * cosines + direction * partner * sines

    query = reordered(rope(stacked(0), 1.0).astype(bf16).astype(f32))
    grad = stacked(cols)
    grad_own = reordered(grad)
    packed_query = jnp.concatenate(
        [jnp.where(first_half, query, 0.0), jnp.where(first_half, turned(query), 0.0)], axis=1
    ).astype(bf16)
    packed_grad = jnp.concatenate(
        [jnp.where(first_half, 0.0, turned(grad_own)), jnp.where(first_half, 0.0, grad_own)],
        axis=1,
    ).astype(bf16)
    key_values = jnp.concatenate([own[...], other[...]], axis=1)
    tokens = key_values.shape[0]
    scores = dot_nt(packed_query, key_values) * scale
    row = lax.broadcasted_iota(jnp.int32, (heads * rows, tokens), 0) % rows + place[1]
    causal = row >= lax.broadcasted_iota(jnp.int32, (heads * rows, tokens), 1)
    scores = jnp.where(causal, scores, -jnp.inf)
    shifted = jnp.exp(scores - jnp.max(scores, axis=1, keepdims=True))
    probs = shifted / jnp.sum(shifted, axis=1, keepdims=True)
    prob_weights = probs.astype(bf16)
    mixed = dot(prob_weights, key_values)
    attention = reordered(
        jnp.where(first_half, turned(mixed[:, :HEAD_DIM]), mixed[:, HEAD_DIM:])
    ).astype(bf16)
    delta = jnp.sum(grad * attention.astype(f32), axis=1, keepdims=True)
    prob_grad = dot_nt(packed_grad, key_values)
    score_grad = (probs * (prob_grad - delta) * scale).astype(bf16)
    mixed = dot(score_grad, key_values)
    query_grad = rope(
        reordered(jnp.where(first_half, mixed[:, :HEAD_DIM], turned(mixed[:, HEAD_DIM:]))), -1.0
    ).astype(bf16)
    key_value_grad = dot_tn(
        jnp.concatenate([score_grad, prob_weights], axis=0),
        jnp.concatenate([packed_query, packed_grad], axis=0),
    )
    kept[...] = key_value_grad[:, :HEAD_DIM]
    given[...] = key_value_grad[:, HEAD_DIM:].astype(bf16)
    low = joint[:, 2 * cols :]
    out_rank = low[:, 3 * ADAPTER_RANK : 4 * ADAPTER_RANK]
    for h in range(heads):
        lanes = slice(h * HEAD_DIM, (h + 1) * HEAD_DIM)
        of_head = attention[h * rows : (h + 1) * rows]
        riding[:, lanes] = query_grad[h * rows : (h + 1) * rows]
        attention_rows[:, lanes] = of_head
        riding[h * ADAPTER_RANK : (h + 1) * ADAPTER_RANK, cols : cols + HEAD_DIM] = dot_tn(
            out_rank, of_head
        ).astype(bf16)
    riding[:, cols + HEAD_DIM :] = low


def shards(
    hidden,
    upstream,
    query_frozen_weight,
    key_value_frozen_weight,
    output_frozen_weight,
    adapter_down,
    query_up_map,
    key_value_up_maps,
    output_down_map,
    output_up,
):
    ffn_count = lax.axis_size("ffn")
    width_count = lax.axis_size("width")
    ffn_index = lax.axis_index("ffn")
    width_index = lax.axis_index("width")
    parity = ffn_index % 2
    same_core = by_core(ffn_count)
    own_rows, width_cols = hidden.shape
    token_count = own_rows * ffn_count
    query_rows = token_count // width_count
    query_cols = query_frozen_weight.shape[1]
    key_cols = key_value_frozen_weight.shape[2]
    heads = query_cols // HEAD_DIM
    rank = ADAPTER_RANK
    score_scale = 1.0 / math.sqrt(HEAD_DIM)
    row_positions = width_index * query_rows + jnp.arange(query_rows, dtype=jnp.int32)

    query_weight = (
        query_frozen_weight.astype(f32) + adapter_scale * dot_tn(adapter_down[0], query_up_map)
    ).astype(bf16)
    key_value_weight = jnp.concatenate(
        [
            key_value_frozen_weight[k].astype(f32)
            + adapter_scale * dot_tn(adapter_down[k + 1], key_value_up_maps[k])
            for k in range(2)
        ],
        axis=1,
    ).astype(bf16)
    output_weight = (
        output_frozen_weight.astype(f32) + adapter_scale * dot_tn(output_down_map, output_up)
    ).astype(bf16)
    down = adapter_down.reshape(3 * rank, width_cols)
    from_hidden = jnp.concatenate(
        [query_weight, jnp.zeros((width_cols, query_cols), bf16), down.T], axis=1
    )
    from_upstream = jnp.concatenate(
        [jnp.zeros((width_cols, query_cols), bf16), output_weight.T], axis=1
    )
    pad = 128
    from_hidden = jnp.pad(from_hidden, ((0, 0), (0, pad - 3 * rank)))
    from_upstream = jnp.concatenate(
        [
            from_upstream,
            jnp.zeros((width_cols, 3 * rank), bf16),
            output_up.T,
            jnp.zeros((width_cols, pad - 4 * rank), bf16),
        ],
        axis=1,
    )
    joint_weight = jnp.concatenate([from_hidden, from_upstream], axis=0)
    query_tables = rope_tables(row_positions, 0, HEAD_DIM)
    key_tables = rope_tables(row_positions, ffn_index * key_cols, key_cols)
    joint_weight, key_value_weight, query_weight, query_tables, key_tables = (
        lax.optimization_barrier(
            (joint_weight, key_value_weight, query_weight, query_tables, key_tables)
        )
    )

    both = jnp.concatenate([hidden, upstream], axis=1)
    own_core = sent_to_all(both, "ffn", same_core)
    other_core = from_partner(own_core)
    rows = jnp.where(
        parity == 0,
        jnp.stack([own_core, other_core], axis=1),
        jnp.stack([other_core, own_core], axis=1),
    ).reshape(token_count, 2 * width_cols)
    hidden_rows = rows[:, :width_cols]
    upstream_rows = rows[:, width_cols:]

    joint_part = dot(rows, joint_weight).astype(bf16)
    joint_rows = lax.psum_scatter(joint_part, "width", scatter_dimension=0, tiled=True)

    key_value_part = dot(hidden_rows, key_value_weight).astype(bf16)
    key_value_sum = pieces_summed(key_value_part, "width")
    key_value_rows = jnp.concatenate(
        [rotate(key_value_sum[:, :key_cols], key_tables, 1.0), key_value_sum[:, key_cols:]], axis=1
    ).astype(bf16)
    own_half = lax.all_gather(key_value_rows, "width", axis=0, tiled=True)
    other_half = from_partner(own_half)

    place = jnp.stack([parity, width_index * query_rows]).astype(jnp.int32)
    vmem = pl.BlockSpec(memory_space=pltpu.VMEM)
    riding, attention_rows, kept, given = pl.pallas_call(
        functools.partial(attention_block, heads=heads, scale=score_scale),
        out_shape=(
            jax.ShapeDtypeStruct((query_rows, query_cols + 2 * HEAD_DIM), bf16),
            jax.ShapeDtypeStruct((query_rows, query_cols), bf16),
            jax.ShapeDtypeStruct((token_count, 2 * key_cols), f32),
            jax.ShapeDtypeStruct((token_count, 2 * key_cols), bf16),
        ),
        in_specs=[pl.BlockSpec(memory_space=pltpu.SMEM)] + [vmem] * 5,
        out_specs=(vmem,) * 4,
        cost_estimate=pl.CostEstimate(
            flops=12 * heads * query_rows * token_count * HEAD_DIM,
            bytes_accessed=2**21,
            transcendentals=heads * query_rows * token_count,
        ),
        name="attention",
    )(place, joint_rows, own_half, other_half, *query_tables)
    query_grad = riding[:, :query_cols]

    gathered = lax.all_gather(riding, "width", axis=0, tiled=True)

    key_value_total = (kept + from_partner(given).astype(f32)).astype(bf16)
    key_value_grad_sum = pieces_summed(key_value_total, "width")
    key_value_grad = jnp.concatenate(
        [
            rotate(key_value_grad_sum[:, :key_cols], key_tables, -1.0),
            key_value_grad_sum[:, key_cols:],
        ],
        axis=1,
    ).astype(bf16)
    terms = jnp.concatenate(
        [
            dot_nt(query_grad, query_up_map),
            dot_nt(key_value_grad[:, :key_cols], key_value_up_maps[0]),
            dot_nt(key_value_grad[:, key_cols:], key_value_up_maps[1]),
            dot_nt(attention_rows, output_down_map),
        ],
        axis=1,
    ).astype(bf16)
    terms = sent_to_all(terms, "ffn").astype(f32).sum(axis=0).astype(bf16)
    key_value_gathered = lax.all_gather(
        jnp.concatenate([key_value_grad, terms], axis=1), "width", axis=0, tiled=True
    )
    key_value_grad_rows = key_value_gathered[:, : 2 * key_cols]

    input_weight = jnp.concatenate([query_weight, key_value_weight], axis=1)

    def input_part(of_core):
        def rows_of(values):
            by_owner = values.reshape(ffn_count // 2, 2, own_rows, -1)
            return lax.dynamic_index_in_dim(by_owner, of_core, 1, keepdims=False)

        grads = jnp.concatenate(
            [rows_of(gathered)[..., :query_cols], rows_of(key_value_grad_rows)], axis=-1
        ).reshape(ffn_count // 2 * own_rows, -1)
        return dot_nt(grads, input_weight)

    given = from_partner(input_part(1 - parity).astype(bf16))
    pair_sum = (input_part(parity) + given.astype(f32)).astype(bf16)
    hidden_gradient = pieces_summed(pair_sum, "ffn", same_core).astype(bf16)

    low = gathered[:, query_cols + HEAD_DIM :]
    rank_gradient = key_value_gathered[:, 2 * key_cols : 2 * key_cols + 3 * rank]
    outer_rank = key_value_gathered[:, 2 * key_cols + 3 * rank :]
    down_map_gradient = (adapter_scale * dot_tn(rank_gradient, hidden_rows)).reshape(
        adapter_down.shape
    )
    query_up_map_gradient = adapter_scale * dot_tn(low[:, :rank], gathered[:, :query_cols])
    key_value_up_maps_gradient = adapter_scale * jnp.stack(
        [
            dot_tn(low[:, rank : 2 * rank], key_value_grad_rows[:, :key_cols]),
            dot_tn(low[:, 2 * rank : 3 * rank], key_value_grad_rows[:, key_cols:]),
        ]
    )
    output_down_sum = (
        gathered[:, query_cols : query_cols + HEAD_DIM]
        .reshape(width_count, heads, rank, HEAD_DIM)
        .astype(f32)
        .sum(axis=0)
    )
    output_down_map_gradient = adapter_scale * output_down_sum.transpose(1, 0, 2).reshape(
        rank, query_cols
    )
    output_up_map_gradient = adapter_scale * dot_tn(outer_rank, upstream_rows)
    return (
        hidden_gradient,
        down_map_gradient,
        query_up_map_gradient,
        key_value_up_maps_gradient,
        output_down_map_gradient,
        output_up_map_gradient,
    )


def solution(mesh):
    placed = (
        P(("groups", "ffn"), "width"),
        P(("groups", "ffn"), "width"),
        P("width", "ffn"),
        P(None, "width", "ffn"),
        P("ffn", "width"),
        P("groups", None, "width"),
        P("groups", "ffn"),
        P("groups", None, "ffn"),
        P("groups", "ffn"),
        P("groups", "width"),
    )
    return jax.shard_map(
        shards,
        mesh=mesh,
        in_specs=placed,
        out_specs=(
            P(("groups", "ffn"), "width"),
            P("groups", None, "width"),
            P("groups", "ffn"),
            P("groups", None, "ffn"),
            P("groups", "ffn"),
            P("groups", "width"),
        ),
        check_vma=False,
    )
```

```python
import functools
import math

import jax
import jax.numpy as jnp
from jax import lax
from jax.experimental import pallas as pl
from jax.experimental.pallas import tpu as pltpu
from jax.sharding import PartitionSpec as P


HEAD_DIM = 128
ADAPTER_RANK = 16

adapter_scale = 2.0
rope_base = 500000.0

f32 = jnp.float32
bf16 = jnp.bfloat16


def dot(a, b):
    return jnp.dot(a, b, preferred_element_type=f32)


def dot_nt(a, b):
    return lax.dot_general(a, b, (((1,), (1,)), ((), ())), preferred_element_type=f32)


def dot_tn(a, b):
    return lax.dot_general(a, b, (((0,), (0,)), ((), ())), preferred_element_type=f32)


def by_core(size):
    return [[2 * k + c for k in range(size // 2)] for c in range(2)]


def from_partner(array):
    return lax.ppermute(array, "ffn", [(i, i ^ 1) for i in range(lax.axis_size("ffn"))])


def sent_to_all(array, axis, groups=None):
    size = len(groups[0]) if groups else lax.axis_size(axis)
    copies = jnp.broadcast_to(array[None], (size, *array.shape))
    return lax.all_to_all(copies, axis, 0, 0, tiled=True, axis_index_groups=groups)


def pieces_summed(array, axis, groups=None):
    size = len(groups[0]) if groups else lax.axis_size(axis)
    pieces = array.reshape(size, array.shape[0] // size, *array.shape[1:])
    arrived = lax.all_to_all(pieces, axis, 0, 0, tiled=True, axis_index_groups=groups)
    return arrived.astype(f32).sum(axis=0)


def rope_tables(positions, first_dim, columns):
    dims = (first_dim + jnp.arange(columns, dtype=jnp.int32)) % HEAD_DIM
    pair_dims = dims - dims % 2
    frequency = jnp.exp(pair_dims.astype(f32) * (-math.log(rope_base) / HEAD_DIM))
    angles = positions.astype(f32)[:, None] * frequency[None, :]
    return jnp.cos(angles), jnp.sin(angles)


def rotate(values, tables, direction):
    cos, sin = tables
    is_even = jnp.arange(values.shape[-1], dtype=jnp.int32) % 2 == 0
    following = jnp.roll(values, -1, axis=-1)
    preceding = jnp.roll(values, 1, axis=-1)
    partner = jnp.where(is_even, -following, preceding)
    return values * cos + direction * partner * sin


def projections(
    place, own, other, query_weight, output_weight, low_weight, key_value_weight, joint, key_value
):
    chips, rows, both = own.shape
    width = both // 2
    cols = query_weight.shape[1]
    grads = output_weight.shape[1]
    for swap, part in enumerate((own, other)):
        core = place[0] if swap == 0 else 1 - place[0]
        tokens = part[...].reshape(chips * rows, both)
        hidden, upstream = tokens[:, :width], tokens[:, width:]
        for value, out, lanes in (
            (dot(hidden, query_weight[...]), joint, slice(0, cols)),
            (dot(upstream, output_weight[...]), joint, slice(cols, cols + grads)),
            (dot(tokens, low_weight[...]), joint, slice(cols + grads, joint.shape[2])),
            (dot(hidden, key_value_weight[...]), key_value, slice(0, key_value.shape[2])),
        ):
            value = value.astype(bf16)
            for chip in range(chips):
                out[2 * chip + core, :, lanes] = value[chip * rows : (chip + 1) * rows]


def attention_block(
    place, joint, own, other, cos, sin, riding, attention_rows, kept, given, *, heads, scale
):
    swapped = place[0] == 1
    rows = joint.shape[0]
    cols = heads * HEAD_DIM
    half = HEAD_DIM // 2

    def stacked(start):
        return jnp.concatenate(
            [joint[:, start + h * HEAD_DIM : start + (h + 1) * HEAD_DIM] for h in range(heads)],
            axis=0,
        ).astype(f32)

    def turned(values):
        return pltpu.roll(values, half, 1)

    def reordered(values):
        return jnp.where(swapped, turned(values), values)

    lane = lax.broadcasted_iota(jnp.int32, (heads * rows, HEAD_DIM), 1)
    first_half = lane < half
    is_even = lane % 2 == 0
    cosines = jnp.concatenate([cos[...]] * heads, axis=0)
    sines = jnp.concatenate([sin[...]] * heads, axis=0)

    def rope(values, direction):
        partner = jnp.where(
            is_even, -pltpu.roll(values, HEAD_DIM - 1, 1), pltpu.roll(values, 1, 1)
        )
        return values * cosines + direction * partner * sines

    query = reordered(rope(stacked(0), 1.0).astype(bf16).astype(f32))
    grad = stacked(cols)
    grad_own = reordered(grad)
    packed_query = jnp.concatenate(
        [jnp.where(first_half, query, 0.0), jnp.where(first_half, turned(query), 0.0)], axis=1
    ).astype(bf16)
    packed_grad = jnp.concatenate(
        [jnp.where(first_half, 0.0, turned(grad_own)), jnp.where(first_half, 0.0, grad_own)],
        axis=1,
    ).astype(bf16)
    key_values = jnp.concatenate([own[...], other[...]], axis=1)
    tokens = key_values.shape[0]
    scores = dot_nt(packed_query, key_values) * scale
    row = lax.broadcasted_iota(jnp.int32, (heads * rows, tokens), 0) % rows + place[1]
    causal = row >= lax.broadcasted_iota(jnp.int32, (heads * rows, tokens), 1)
    scores = jnp.where(causal, scores, -jnp.inf)
    shifted = jnp.exp(scores - jnp.max(scores, axis=1, keepdims=True))
    probs = shifted / jnp.sum(shifted, axis=1, keepdims=True)
    prob_weights = probs.astype(bf16)
    mixed = dot(prob_weights, key_values)
    attention = reordered(
        jnp.where(first_half, turned(mixed[:, :HEAD_DIM]), mixed[:, HEAD_DIM:])
    ).astype(bf16)
    delta = jnp.sum(grad * attention.astype(f32), axis=1, keepdims=True)
    prob_grad = dot_nt(packed_grad, key_values)
    score_grad = (probs * (prob_grad - delta) * scale).astype(bf16)
    mixed = dot(score_grad, key_values)
    query_grad = rope(
        reordered(jnp.where(first_half, mixed[:, :HEAD_DIM], turned(mixed[:, HEAD_DIM:]))), -1.0
    ).astype(bf16)
    key_value_grad = dot_tn(
        jnp.concatenate([score_grad, prob_weights], axis=0),
        jnp.concatenate([packed_query, packed_grad], axis=0),
    )
    kept[...] = key_value_grad[:, :HEAD_DIM]
    given[...] = key_value_grad[:, HEAD_DIM:].astype(bf16)
    low = joint[:, 2 * cols :]
    out_rank = low[:, 3 * ADAPTER_RANK : 4 * ADAPTER_RANK]
    for h in range(heads):
        lanes = slice(h * HEAD_DIM, (h + 1) * HEAD_DIM)
        of_head = attention[h * rows : (h + 1) * rows]
        riding[:, lanes] = query_grad[h * rows : (h + 1) * rows]
        attention_rows[:, lanes] = of_head
        riding[h * ADAPTER_RANK : (h + 1) * ADAPTER_RANK, cols : cols + HEAD_DIM] = dot_tn(
            out_rank, of_head
        ).astype(bf16)
    riding[:, cols + HEAD_DIM :] = low


def shards(
    hidden,
    upstream,
    query_frozen_weight,
    key_value_frozen_weight,
    output_frozen_weight,
    adapter_down,
    query_up_map,
    key_value_up_maps,
    output_down_map,
    output_up,
):
    ffn_count = lax.axis_size("ffn")
    width_count = lax.axis_size("width")
    ffn_index = lax.axis_index("ffn")
    width_index = lax.axis_index("width")
    parity = ffn_index % 2
    same_core = by_core(ffn_count)
    own_rows, width_cols = hidden.shape
    token_count = own_rows * ffn_count
    query_rows = token_count // width_count
    query_cols = query_frozen_weight.shape[1]
    key_cols = key_value_frozen_weight.shape[2]
    heads = query_cols // HEAD_DIM
    rank = ADAPTER_RANK
    score_scale = 1.0 / math.sqrt(HEAD_DIM)
    row_positions = width_index * query_rows + jnp.arange(query_rows, dtype=jnp.int32)

    query_weight = (
        query_frozen_weight.astype(f32) + adapter_scale * dot_tn(adapter_down[0], query_up_map)
    ).astype(bf16)
    key_value_weight = jnp.concatenate(
        [
            key_value_frozen_weight[k].astype(f32)
            + adapter_scale * dot_tn(adapter_down[k + 1], key_value_up_maps[k])
            for k in range(2)
        ],
        axis=1,
    ).astype(bf16)
    output_weight = (
        output_frozen_weight.astype(f32) + adapter_scale * dot_tn(output_down_map, output_up)
    ).astype(bf16)
    down = adapter_down.reshape(3 * rank, width_cols)
    low_weight = jnp.concatenate(
        [
            jnp.pad(down, ((0, HEAD_DIM - 3 * rank), (0, 0))),
            jnp.pad(output_up, ((3 * rank, HEAD_DIM - 4 * rank), (0, 0))),
        ],
        axis=1,
    ).T
    output_weight = output_weight.T
    query_tables = rope_tables(row_positions, 0, HEAD_DIM)
    key_tables = rope_tables(row_positions, ffn_index * key_cols, key_cols)
    low_weight, output_weight, key_value_weight, query_weight, query_tables, key_tables = (
        lax.optimization_barrier(
            (low_weight, output_weight, key_value_weight, query_weight, query_tables, key_tables)
        )
    )

    both = jnp.concatenate([hidden, upstream], axis=1)
    own_core = sent_to_all(both, "ffn", same_core)
    other_core = from_partner(own_core)
    rows = jnp.where(
        parity == 0,
        jnp.stack([own_core, other_core], axis=1),
        jnp.stack([other_core, own_core], axis=1),
    ).reshape(token_count, 2 * width_cols)
    hidden_rows = rows[:, :width_cols]
    upstream_rows = rows[:, width_cols:]

    place = jnp.stack([parity, width_index * query_rows]).astype(jnp.int32)
    smem = pl.BlockSpec(memory_space=pltpu.SMEM)
    vmem = pl.BlockSpec(memory_space=pltpu.VMEM)
    joint_part, key_value_part = pl.pallas_call(
        projections,
        out_shape=(
            jax.ShapeDtypeStruct((ffn_count, own_rows, 2 * query_cols + HEAD_DIM), bf16),
            jax.ShapeDtypeStruct((ffn_count, own_rows, 2 * key_cols), bf16),
        ),
        in_specs=[smem] + [vmem] * 6,
        out_specs=(vmem, vmem),
        cost_estimate=pl.CostEstimate(
            flops=2 * token_count * width_cols * (2 * query_cols + 2 * HEAD_DIM),
            bytes_accessed=2**23,
            transcendentals=0,
        ),
        name="projections",
    )(place, own_core, other_core, query_weight, output_weight, low_weight, key_value_weight)
    joint_part = joint_part.reshape(token_count, -1)
    key_value_part = key_value_part.reshape(token_count, -1)
    joint_rows = lax.psum_scatter(joint_part, "width", scatter_dimension=0, tiled=True)

    key_value_sum = pieces_summed(key_value_part, "width")
    key_value_rows = jnp.concatenate(
        [rotate(key_value_sum[:, :key_cols], key_tables, 1.0), key_value_sum[:, key_cols:]], axis=1
    ).astype(bf16)
    own_half = lax.all_gather(key_value_rows, "width", axis=0, tiled=True)
    other_half = from_partner(own_half)

    riding, attention_rows, kept, given = pl.pallas_call(
        functools.partial(attention_block, heads=heads, scale=score_scale),
        out_shape=(
            jax.ShapeDtypeStruct((query_rows, query_cols + 2 * HEAD_DIM), bf16),
            jax.ShapeDtypeStruct((query_rows, query_cols), bf16),
            jax.ShapeDtypeStruct((token_count, 2 * key_cols), f32),
            jax.ShapeDtypeStruct((token_count, 2 * key_cols), bf16),
        ),
        in_specs=[smem] + [vmem] * 5,
        out_specs=(vmem,) * 4,
        cost_estimate=pl.CostEstimate(
            flops=12 * heads * query_rows * token_count * HEAD_DIM,
            bytes_accessed=2**21,
            transcendentals=heads * query_rows * token_count,
        ),
        name="attention",
    )(place, joint_rows, own_half, other_half, *query_tables)
    query_grad = riding[:, :query_cols]

    gathered = lax.all_gather(riding, "width", axis=0, tiled=True)

    key_value_total = (kept + from_partner(given).astype(f32)).astype(bf16)
    terms = jnp.concatenate(
        [dot_nt(query_grad, query_up_map), dot_nt(attention_rows, output_down_map)], axis=1
    ).astype(bf16)
    key_value_total, terms = lax.optimization_barrier((key_value_total, terms))
    key_value_grad_sum = pieces_summed(key_value_total, "width")
    terms = lax.all_gather(terms, "ffn").astype(f32).sum(axis=0).astype(bf16)
    key_value_grad = jnp.concatenate(
        [
            rotate(key_value_grad_sum[:, :key_cols], key_tables, -1.0),
            key_value_grad_sum[:, key_cols:],
        ],
        axis=1,
    ).astype(bf16)
    key_value_gathered = lax.all_gather(
        jnp.concatenate([key_value_grad, terms], axis=1), "width", axis=0, tiled=True
    )
    key_value_grad_rows = key_value_gathered[:, : 2 * key_cols]
    key_value_terms = jnp.concatenate(
        [
            dot_nt(key_value_grad_rows[:, :key_cols], key_value_up_maps[0]),
            dot_nt(key_value_grad_rows[:, key_cols:], key_value_up_maps[1]),
        ],
        axis=1,
    ).astype(bf16)
    key_value_down = dot_tn(key_value_terms, hidden_rows)
    key_value_down = (key_value_down + from_partner(key_value_down)).astype(bf16)
    key_value_down = sent_to_all(key_value_down, "ffn", same_core).astype(f32).sum(axis=0)

    input_weight = jnp.concatenate([query_weight, key_value_weight], axis=1)

    def input_part(of_core):
        def rows_of(values):
            by_owner = values.reshape(ffn_count // 2, 2, own_rows, -1)
            return lax.dynamic_index_in_dim(by_owner, of_core, 1, keepdims=False)

        grads = jnp.concatenate(
            [rows_of(gathered)[..., :query_cols], rows_of(key_value_grad_rows)], axis=-1
        ).reshape(ffn_count // 2 * own_rows, -1)
        return dot_nt(grads, input_weight)

    given = from_partner(input_part(1 - parity).astype(bf16))
    pair_sum = (input_part(parity) + given.astype(f32)).astype(bf16)
    hidden_gradient = pieces_summed(pair_sum, "ffn", same_core).astype(bf16)

    low = gathered[:, query_cols + HEAD_DIM :]
    query_rank = key_value_gathered[:, 2 * key_cols : 2 * key_cols + rank]
    outer_rank = key_value_gathered[:, 2 * key_cols + rank :]
    down_map_gradient = adapter_scale * jnp.concatenate(
        [dot_tn(query_rank, hidden_rows), key_value_down], axis=0
    ).reshape(adapter_down.shape)
    query_up_map_gradient = adapter_scale * dot_tn(low[:, :rank], gathered[:, :query_cols])
    key_value_up_maps_gradient = adapter_scale * jnp.stack(
        [
            dot_tn(low[:, rank : 2 * rank], key_value_grad_rows[:, :key_cols]),
            dot_tn(low[:, 2 * rank : 3 * rank], key_value_grad_rows[:, key_cols:]),
        ]
    )
    output_down_sum = (
        gathered[:, query_cols : query_cols + HEAD_DIM]
        .reshape(width_count, heads, rank, HEAD_DIM)
        .astype(f32)
        .sum(axis=0)
    )
    output_down_map_gradient = adapter_scale * output_down_sum.transpose(1, 0, 2).reshape(
        rank, query_cols
    )
    output_up_map_gradient = adapter_scale * dot_tn(outer_rank, upstream_rows)
    return (
        hidden_gradient,
        down_map_gradient,
        query_up_map_gradient,
        key_value_up_maps_gradient,
        output_down_map_gradient,
        output_up_map_gradient,
    )


def solution(mesh):
    placed = (
        P(("groups", "ffn"), "width"),
        P(("groups", "ffn"), "width"),
        P("width", "ffn"),
        P(None, "width", "ffn"),
        P("ffn", "width"),
        P("groups", None, "width"),
        P("groups", "ffn"),
        P("groups", None, "ffn"),
        P("groups", "ffn"),
        P("groups", "width"),
    )
    return jax.shard_map(
        shards,
        mesh=mesh,
        in_specs=placed,
        out_specs=(
            P(("groups", "ffn"), "width"),
            P("groups", None, "width"),
            P("groups", "ffn"),
            P("groups", None, "ffn"),
            P("groups", "ffn"),
            P("groups", "width"),
        ),
        check_vma=False,
    )
```

```python
import functools
import math

import jax
import jax.numpy as jnp
from jax import lax
from jax.experimental import pallas as pl
from jax.experimental.pallas import tpu as pltpu
from jax.sharding import PartitionSpec as P


HEAD_DIM = 128
ADAPTER_RANK = 16

adapter_scale = 2.0
rope_base = 500000.0

f32 = jnp.float32
bf16 = jnp.bfloat16


def dot(a, b):
    return jnp.dot(a, b, preferred_element_type=f32)


def dot_nt(a, b):
    return lax.dot_general(a, b, (((1,), (1,)), ((), ())), preferred_element_type=f32)


def dot_tn(a, b):
    return lax.dot_general(a, b, (((0,), (0,)), ((), ())), preferred_element_type=f32)


def by_core(size):
    return [[2 * k + c for k in range(size // 2)] for c in range(2)]


def from_partner(array):
    return lax.ppermute(array, "ffn", [(i, i ^ 1) for i in range(lax.axis_size("ffn"))])


def sent_to_all(array, axis, groups=None):
    size = len(groups[0]) if groups else lax.axis_size(axis)
    copies = jnp.broadcast_to(array[None], (size, *array.shape))
    return lax.all_to_all(copies, axis, 0, 0, tiled=True, axis_index_groups=groups)


def pieces_summed(array, axis, groups=None):
    size = len(groups[0]) if groups else lax.axis_size(axis)
    pieces = array.reshape(size, array.shape[0] // size, *array.shape[1:])
    arrived = lax.all_to_all(pieces, axis, 0, 0, tiled=True, axis_index_groups=groups)
    return arrived.astype(f32).sum(axis=0)


def rope_tables(positions, first_dim, columns):
    dims = (first_dim + jnp.arange(columns, dtype=jnp.int32)) % HEAD_DIM
    pair_dims = dims - dims % 2
    frequency = jnp.exp(pair_dims.astype(f32) * (-math.log(rope_base) / HEAD_DIM))
    angles = positions.astype(f32)[:, None] * frequency[None, :]
    return jnp.cos(angles), jnp.sin(angles)


def rotate(values, tables, direction):
    cos, sin = tables
    is_even = jnp.arange(values.shape[-1], dtype=jnp.int32) % 2 == 0
    following = jnp.roll(values, -1, axis=-1)
    preceding = jnp.roll(values, 1, axis=-1)
    partner = jnp.where(is_even, -following, preceding)
    return values * cos + direction * partner * sin


def projected(part, query_weight, output_weight, low_weight, key_value_weight):
    chips, rows, both = part.shape
    tokens = part[...].reshape(chips * rows, both)
    hidden, upstream = tokens[:, : both // 2], tokens[:, both // 2 :]
    cols = query_weight.shape[1]
    end = cols + output_weight.shape[1]
    joint = (
        (dot(hidden, query_weight[...]).astype(bf16), slice(0, cols)),
        (dot(upstream, output_weight[...]).astype(bf16), slice(cols, end)),
        (dot(tokens, low_weight[...]).astype(bf16), slice(end, end + low_weight.shape[1])),
    )
    return joint, dot(hidden, key_value_weight[...]).astype(bf16)


def own_projections(
    own, query_weight, output_weight, low_weight, key_value_weight, joint, key_value
):
    values, of_key_value = projected(
        own, query_weight, output_weight, low_weight, key_value_weight
    )
    for value, lanes in values:
        joint[:, :, lanes] = value.reshape(*own.shape[:2], -1)
    key_value[...] = of_key_value.reshape(key_value.shape)


def all_projections(
    place,
    other,
    query_weight,
    output_weight,
    low_weight,
    key_value_weight,
    own_joint,
    own_key_value,
    joint,
    key_value,
):
    chips, rows, _ = other.shape
    values, of_key_value = projected(
        other, query_weight, output_weight, low_weight, key_value_weight
    )
    core = place[0]
    for chip in range(chips):
        here = slice(chip * rows, (chip + 1) * rows)
        joint[2 * chip + core] = own_joint[chip]
        key_value[2 * chip + core] = own_key_value[chip]
        for value, lanes in values:
            joint[2 * chip + 1 - core, :, lanes] = value[here]
        key_value[2 * chip + 1 - core] = of_key_value[here]


def attention_block(
    place, joint, own, other, cos, sin, riding, attention_rows, kept, given, *, heads, scale
):
    swapped = place[0] == 1
    rows = joint.shape[0]
    cols = heads * HEAD_DIM
    half = HEAD_DIM // 2

    def stacked(start):
        return jnp.concatenate(
            [joint[:, start + h * HEAD_DIM : start + (h + 1) * HEAD_DIM] for h in range(heads)],
            axis=0,
        ).astype(f32)

    def turned(values):
        return pltpu.roll(values, half, 1)

    def reordered(values):
        return jnp.where(swapped, turned(values), values)

    lane = lax.broadcasted_iota(jnp.int32, (heads * rows, HEAD_DIM), 1)
    first_half = lane < half
    is_even = lane % 2 == 0
    cosines = jnp.concatenate([cos[...]] * heads, axis=0)
    sines = jnp.concatenate([sin[...]] * heads, axis=0)

    def rope(values, direction):
        partner = jnp.where(
            is_even, -pltpu.roll(values, HEAD_DIM - 1, 1), pltpu.roll(values, 1, 1)
        )
        return values * cosines + direction * partner * sines

    query = reordered(rope(stacked(0), 1.0).astype(bf16).astype(f32))
    grad = stacked(cols)
    grad_own = reordered(grad)
    packed_query = jnp.concatenate(
        [jnp.where(first_half, query, 0.0), jnp.where(first_half, turned(query), 0.0)], axis=1
    ).astype(bf16)
    packed_grad = jnp.concatenate(
        [jnp.where(first_half, 0.0, turned(grad_own)), jnp.where(first_half, 0.0, grad_own)],
        axis=1,
    ).astype(bf16)
    key_values = jnp.concatenate([own[...], other[...]], axis=1)
    tokens = key_values.shape[0]
    scores = dot_nt(packed_query, key_values) * scale
    row = lax.broadcasted_iota(jnp.int32, (heads * rows, tokens), 0) % rows + place[1]
    causal = row >= lax.broadcasted_iota(jnp.int32, (heads * rows, tokens), 1)
    scores = jnp.where(causal, scores, -jnp.inf)
    shifted = jnp.exp(scores - jnp.max(scores, axis=1, keepdims=True))
    probs = shifted / jnp.sum(shifted, axis=1, keepdims=True)
    prob_weights = probs.astype(bf16)
    mixed = dot(prob_weights, key_values)
    attention = reordered(
        jnp.where(first_half, turned(mixed[:, :HEAD_DIM]), mixed[:, HEAD_DIM:])
    ).astype(bf16)
    delta = jnp.sum(grad * attention.astype(f32), axis=1, keepdims=True)
    prob_grad = dot_nt(packed_grad, key_values)
    score_grad = (probs * (prob_grad - delta) * scale).astype(bf16)
    mixed = dot(score_grad, key_values)
    query_grad = rope(
        reordered(jnp.where(first_half, mixed[:, :HEAD_DIM], turned(mixed[:, HEAD_DIM:]))), -1.0
    ).astype(bf16)
    key_value_grad = dot_tn(
        jnp.concatenate([score_grad, prob_weights], axis=0),
        jnp.concatenate([packed_query, packed_grad], axis=0),
    )
    kept[...] = key_value_grad[:, :HEAD_DIM]
    given[...] = key_value_grad[:, HEAD_DIM:].astype(bf16)
    low = joint[:, 2 * cols :]
    out_rank = low[:, 3 * ADAPTER_RANK : 4 * ADAPTER_RANK]
    for h in range(heads):
        lanes = slice(h * HEAD_DIM, (h + 1) * HEAD_DIM)
        of_head = attention[h * rows : (h + 1) * rows]
        riding[:, lanes] = query_grad[h * rows : (h + 1) * rows]
        attention_rows[:, lanes] = of_head
        riding[h * ADAPTER_RANK : (h + 1) * ADAPTER_RANK, cols : cols + HEAD_DIM] = dot_tn(
            out_rank, of_head
        ).astype(bf16)
    riding[:, cols + HEAD_DIM :] = low


def shards(
    hidden,
    upstream,
    query_frozen_weight,
    key_value_frozen_weight,
    output_frozen_weight,
    adapter_down,
    query_up_map,
    key_value_up_maps,
    output_down_map,
    output_up,
):
    ffn_count = lax.axis_size("ffn")
    width_count = lax.axis_size("width")
    ffn_index = lax.axis_index("ffn")
    width_index = lax.axis_index("width")
    parity = ffn_index % 2
    same_core = by_core(ffn_count)
    own_rows, width_cols = hidden.shape
    token_count = own_rows * ffn_count
    query_rows = token_count // width_count
    query_cols = query_frozen_weight.shape[1]
    key_cols = key_value_frozen_weight.shape[2]
    heads = query_cols // HEAD_DIM
    rank = ADAPTER_RANK
    score_scale = 1.0 / math.sqrt(HEAD_DIM)
    row_positions = width_index * query_rows + jnp.arange(query_rows, dtype=jnp.int32)

    query_weight = (
        query_frozen_weight.astype(f32) + adapter_scale * dot_tn(adapter_down[0], query_up_map)
    ).astype(bf16)
    key_value_weight = jnp.concatenate(
        [
            key_value_frozen_weight[k].astype(f32)
            + adapter_scale * dot_tn(adapter_down[k + 1], key_value_up_maps[k])
            for k in range(2)
        ],
        axis=1,
    ).astype(bf16)
    output_weight = (
        output_frozen_weight.astype(f32) + adapter_scale * dot_tn(output_down_map, output_up)
    ).astype(bf16)
    down = adapter_down.reshape(3 * rank, width_cols)
    low_weight = jnp.concatenate(
        [
            jnp.pad(down, ((0, HEAD_DIM - 3 * rank), (0, 0))),
            jnp.pad(output_up, ((3 * rank, HEAD_DIM - 4 * rank), (0, 0))),
        ],
        axis=1,
    ).T
    output_weight = output_weight.T
    query_tables = rope_tables(row_positions, 0, HEAD_DIM)
    key_tables = rope_tables(row_positions, ffn_index * key_cols, key_cols)
    input_weight = jnp.concatenate([query_weight, key_value_weight], axis=1)
    input_weight, query_tables, key_tables = lax.optimization_barrier(
        (input_weight, query_tables, key_tables)
    )

    both = jnp.concatenate([hidden, upstream], axis=1)
    own_core = sent_to_all(both, "ffn", same_core)
    own_core, low_weight, output_weight, key_value_weight, query_weight = lax.optimization_barrier(
        (own_core, low_weight, output_weight, key_value_weight, query_weight)
    )
    other_core = from_partner(own_core)
    rows = jnp.where(
        parity == 0,
        jnp.stack([own_core, other_core], axis=1),
        jnp.stack([other_core, own_core], axis=1),
    ).reshape(token_count, 2 * width_cols)
    hidden_rows = rows[:, :width_cols]
    upstream_rows = rows[:, width_cols:]

    place = jnp.stack([parity, width_index * query_rows]).astype(jnp.int32)
    smem = pl.BlockSpec(memory_space=pltpu.SMEM)
    vmem = pl.BlockSpec(memory_space=pltpu.VMEM)
    weights = (query_weight, output_weight, low_weight, key_value_weight)

    def of_blocks(blocks):
        return (
            jax.ShapeDtypeStruct((blocks, own_rows, 2 * query_cols + HEAD_DIM), bf16),
            jax.ShapeDtypeStruct((blocks, own_rows, 2 * key_cols), bf16),
        )

    cost = pl.CostEstimate(
        flops=token_count * width_cols * (2 * query_cols + 2 * HEAD_DIM),
        bytes_accessed=2**22,
        transcendentals=0,
    )
    own_parts = pl.pallas_call(
        own_projections,
        out_shape=of_blocks(ffn_count // 2),
        in_specs=[vmem] * 5,
        out_specs=(vmem, vmem),
        cost_estimate=cost,
        compiler_params=pltpu.CompilerParams(vmem_limit_bytes=20 * 2**20),
        name="own_projections",
    )(own_core, *weights)
    joint_part, key_value_part = pl.pallas_call(
        all_projections,
        out_shape=of_blocks(ffn_count),
        in_specs=[smem] + [vmem] * 7,
        out_specs=(vmem, vmem),
        cost_estimate=cost,
        compiler_params=pltpu.CompilerParams(vmem_limit_bytes=20 * 2**20),
        name="all_projections",
    )(place, other_core, *weights, *own_parts)
    joint_part = joint_part.reshape(token_count, -1)
    key_value_part = key_value_part.reshape(token_count, -1)
    joint_rows = lax.psum_scatter(joint_part, "width", scatter_dimension=0, tiled=True)

    key_value_sum = pieces_summed(key_value_part, "width")
    key_value_rows = jnp.concatenate(
        [rotate(key_value_sum[:, :key_cols], key_tables, 1.0), key_value_sum[:, key_cols:]], axis=1
    ).astype(bf16)
    own_half = lax.all_gather(key_value_rows, "width", axis=0, tiled=True)
    other_half = from_partner(own_half)

    riding, attention_rows, kept, given = pl.pallas_call(
        functools.partial(attention_block, heads=heads, scale=score_scale),
        out_shape=(
            jax.ShapeDtypeStruct((query_rows, query_cols + 2 * HEAD_DIM), bf16),
            jax.ShapeDtypeStruct((query_rows, query_cols), bf16),
            jax.ShapeDtypeStruct((token_count, 2 * key_cols), f32),
            jax.ShapeDtypeStruct((token_count, 2 * key_cols), bf16),
        ),
        in_specs=[smem] + [vmem] * 5,
        out_specs=(vmem,) * 4,
        cost_estimate=pl.CostEstimate(
            flops=12 * heads * query_rows * token_count * HEAD_DIM,
            bytes_accessed=2**21,
            transcendentals=heads * query_rows * token_count,
        ),
        compiler_params=pltpu.CompilerParams(vmem_limit_bytes=24 * 2**20),
        name="attention",
    )(place, joint_rows, own_half, other_half, *query_tables)
    query_grad = riding[:, :query_cols]

    gathered = lax.all_gather(riding, "width", axis=0, tiled=True)

    key_value_total = (kept + from_partner(given).astype(f32)).astype(bf16)
    terms = jnp.concatenate(
        [dot_nt(query_grad, query_up_map), dot_nt(attention_rows, output_down_map)], axis=1
    ).astype(bf16)
    key_value_total, terms = lax.optimization_barrier((key_value_total, terms))
    key_value_grad_sum = pieces_summed(key_value_total, "width")
    terms = lax.all_gather(terms, "ffn").astype(f32).sum(axis=0).astype(bf16)
    key_value_grad = jnp.concatenate(
        [
            rotate(key_value_grad_sum[:, :key_cols], key_tables, -1.0),
            key_value_grad_sum[:, key_cols:],
        ],
        axis=1,
    ).astype(bf16)
    key_value_gathered = lax.all_gather(
        jnp.concatenate([key_value_grad, terms], axis=1), "width", axis=0, tiled=True
    )
    key_value_grad_rows = key_value_gathered[:, : 2 * key_cols]
    key_value_terms = jnp.concatenate(
        [
            dot_nt(key_value_grad_rows[:, :key_cols], key_value_up_maps[0]),
            dot_nt(key_value_grad_rows[:, key_cols:], key_value_up_maps[1]),
        ],
        axis=1,
    ).astype(bf16)
    key_value_down = dot_tn(key_value_terms, hidden_rows)
    key_value_down = (key_value_down + from_partner(key_value_down)).astype(bf16)

    def input_part(of_core):
        def rows_of(values):
            by_owner = values.reshape(ffn_count // 2, 2, own_rows, -1)
            return lax.dynamic_index_in_dim(by_owner, of_core, 1, keepdims=False)

        grads = jnp.concatenate(
            [rows_of(gathered)[..., :query_cols], rows_of(key_value_grad_rows)], axis=-1
        ).reshape(ffn_count // 2 * own_rows, -1)
        return dot_nt(grads, input_weight)

    given = from_partner(input_part(1 - parity).astype(bf16))
    pair_sum = (input_part(parity) + given.astype(f32)).astype(bf16)
    pair_sum, key_value_down = lax.optimization_barrier((pair_sum, key_value_down))
    hidden_gradient = pieces_summed(pair_sum, "ffn", same_core).astype(bf16)
    key_value_down = lax.all_gather(key_value_down, "ffn", axis_index_groups=same_core)
    key_value_down = key_value_down.astype(f32).sum(axis=0)

    low = gathered[:, query_cols + HEAD_DIM :]
    query_rank = key_value_gathered[:, 2 * key_cols : 2 * key_cols + rank]
    outer_rank = key_value_gathered[:, 2 * key_cols + rank :]
    down_map_gradient = adapter_scale * jnp.concatenate(
        [dot_tn(query_rank, hidden_rows), key_value_down], axis=0
    ).reshape(adapter_down.shape)
    query_up_map_gradient = adapter_scale * dot_tn(low[:, :rank], gathered[:, :query_cols])
    key_value_up_maps_gradient = adapter_scale * jnp.stack(
        [
            dot_tn(low[:, rank : 2 * rank], key_value_grad_rows[:, :key_cols]),
            dot_tn(low[:, 2 * rank : 3 * rank], key_value_grad_rows[:, key_cols:]),
        ]
    )
    output_down_sum = (
        gathered[:, query_cols : query_cols + HEAD_DIM]
        .reshape(width_count, heads, rank, HEAD_DIM)
        .astype(f32)
        .sum(axis=0)
    )
    output_down_map_gradient = adapter_scale * output_down_sum.transpose(1, 0, 2).reshape(
        rank, query_cols
    )
    output_up_map_gradient = adapter_scale * dot_tn(outer_rank, upstream_rows)
    return (
        hidden_gradient,
        down_map_gradient,
        query_up_map_gradient,
        key_value_up_maps_gradient,
        output_down_map_gradient,
        output_up_map_gradient,
    )


def solution(mesh):
    placed = (
        P(("groups", "ffn"), "width"),
        P(("groups", "ffn"), "width"),
        P("width", "ffn"),
        P(None, "width", "ffn"),
        P("ffn", "width"),
        P("groups", None, "width"),
        P("groups", "ffn"),
        P("groups", None, "ffn"),
        P("groups", "ffn"),
        P("groups", "width"),
    )
    return jax.shard_map(
        shards,
        mesh=mesh,
        in_specs=placed,
        out_specs=(
            P(("groups", "ffn"), "width"),
            P("groups", None, "width"),
            P("groups", "ffn"),
            P("groups", None, "ffn"),
            P("groups", "ffn"),
            P("groups", "width"),
        ),
        check_vma=False,
    )
```

```python
import functools
import math

import jax
import jax.numpy as jnp
from jax import lax
from jax.experimental import pallas as pl
from jax.experimental.pallas import tpu as pltpu
from jax.sharding import PartitionSpec as P


HEAD_DIM = 128
ADAPTER_RANK = 16

adapter_scale = 2.0
rope_base = 500000.0

f32 = jnp.float32
bf16 = jnp.bfloat16


def dot(a, b):
    return jnp.dot(a, b, preferred_element_type=f32)


def dot_nt(a, b):
    return lax.dot_general(a, b, (((1,), (1,)), ((), ())), preferred_element_type=f32)


def dot_tn(a, b):
    return lax.dot_general(a, b, (((0,), (0,)), ((), ())), preferred_element_type=f32)


def by_core(size):
    return [[2 * k + c for k in range(size // 2)] for c in range(2)]


def exchanged(array, step):
    return lax.ppermute(array, "ffn", [(i, i ^ step) for i in range(lax.axis_size("ffn"))])


def from_partner(array):
    return exchanged(array, 1)


def sent_to_all(array, axis, groups=None):
    size = len(groups[0]) if groups else lax.axis_size(axis)
    copies = jnp.broadcast_to(array[None], (size, *array.shape))
    return lax.all_to_all(copies, axis, 0, 0, tiled=True, axis_index_groups=groups)


def pieces_summed(array, axis, groups=None):
    size = len(groups[0]) if groups else lax.axis_size(axis)
    pieces = array.reshape(size, array.shape[0] // size, *array.shape[1:])
    arrived = lax.all_to_all(pieces, axis, 0, 0, tiled=True, axis_index_groups=groups)
    return arrived.astype(f32).sum(axis=0)


def rope_tables(positions, first_dim, columns):
    dims = (first_dim + jnp.arange(columns, dtype=jnp.int32)) % HEAD_DIM
    pair_dims = dims - dims % 2
    frequency = jnp.exp(pair_dims.astype(f32) * (-math.log(rope_base) / HEAD_DIM))
    angles = positions.astype(f32)[:, None] * frequency[None, :]
    return jnp.cos(angles), jnp.sin(angles)


def rotate(values, tables, direction):
    cos, sin = tables
    is_even = jnp.arange(values.shape[-1], dtype=jnp.int32) % 2 == 0
    following = jnp.roll(values, -1, axis=-1)
    preceding = jnp.roll(values, 1, axis=-1)
    partner = jnp.where(is_even, -following, preceding)
    return values * cos + direction * partner * sin


def projected(part, query_weight, output_weight, low_weight, key_value_weight):
    chips, rows, both = part.shape
    tokens = part[...].reshape(chips * rows, both)
    hidden, upstream = tokens[:, : both // 2], tokens[:, both // 2 :]
    cols = query_weight.shape[1]
    end = cols + output_weight.shape[1]
    joint = (
        (dot(hidden, query_weight[...]).astype(bf16), slice(0, cols)),
        (dot(upstream, output_weight[...]).astype(bf16), slice(cols, end)),
        (dot(tokens, low_weight[...]).astype(bf16), slice(end, end + low_weight.shape[1])),
    )
    return joint, dot(hidden, key_value_weight[...]).astype(bf16)


def own_projections(
    own, query_weight, output_weight, low_weight, key_value_weight, joint, key_value
):
    values, of_key_value = projected(
        own, query_weight, output_weight, low_weight, key_value_weight
    )
    for value, lanes in values:
        joint[:, :, lanes] = value.reshape(*own.shape[:2], -1)
    key_value[...] = of_key_value.reshape(key_value.shape)


def all_projections(
    place,
    other,
    query_weight,
    output_weight,
    low_weight,
    key_value_weight,
    own_joint,
    own_key_value,
    joint,
    key_value,
):
    chips, rows, _ = other.shape
    values, of_key_value = projected(
        other, query_weight, output_weight, low_weight, key_value_weight
    )
    core = place[0]
    for chip in range(chips):
        here = slice(chip * rows, (chip + 1) * rows)
        joint[2 * chip + core] = own_joint[chip]
        key_value[2 * chip + core] = own_key_value[chip]
        for value, lanes in values:
            joint[2 * chip + 1 - core, :, lanes] = value[here]
        key_value[2 * chip + 1 - core] = of_key_value[here]


def attention_block(
    place, joint, own, other, cos, sin, riding, attention_rows, kept, given, *, heads, scale
):
    swapped = place[0] == 1
    rows = joint.shape[0]
    cols = heads * HEAD_DIM
    half = HEAD_DIM // 2

    def stacked(start):
        return jnp.concatenate(
            [joint[:, start + h * HEAD_DIM : start + (h + 1) * HEAD_DIM] for h in range(heads)],
            axis=0,
        ).astype(f32)

    def turned(values):
        return pltpu.roll(values, half, 1)

    def reordered(values):
        return jnp.where(swapped, turned(values), values)

    lane = lax.broadcasted_iota(jnp.int32, (heads * rows, HEAD_DIM), 1)
    first_half = lane < half
    is_even = lane % 2 == 0
    cosines = jnp.concatenate([cos[...]] * heads, axis=0)
    sines = jnp.concatenate([sin[...]] * heads, axis=0)

    def rope(values, direction):
        partner = jnp.where(
            is_even, -pltpu.roll(values, HEAD_DIM - 1, 1), pltpu.roll(values, 1, 1)
        )
        return values * cosines + direction * partner * sines

    query = reordered(rope(stacked(0), 1.0).astype(bf16).astype(f32))
    grad = stacked(cols)
    grad_own = reordered(grad)
    packed_query = jnp.concatenate(
        [jnp.where(first_half, query, 0.0), jnp.where(first_half, turned(query), 0.0)], axis=1
    ).astype(bf16)
    packed_grad = jnp.concatenate(
        [jnp.where(first_half, 0.0, turned(grad_own)), jnp.where(first_half, 0.0, grad_own)],
        axis=1,
    ).astype(bf16)
    key_values = jnp.concatenate([own[...], other[...]], axis=1)
    tokens = key_values.shape[0]
    scores = dot_nt(packed_query, key_values) * scale
    row = lax.broadcasted_iota(jnp.int32, (heads * rows, tokens), 0) % rows + place[1]
    causal = row >= lax.broadcasted_iota(jnp.int32, (heads * rows, tokens), 1)
    scores = jnp.where(causal, scores, -jnp.inf)
    shifted = jnp.exp(scores - jnp.max(scores, axis=1, keepdims=True))
    probs = shifted / jnp.sum(shifted, axis=1, keepdims=True)
    prob_weights = probs.astype(bf16)
    mixed = dot(prob_weights, key_values)
    attention = reordered(
        jnp.where(first_half, turned(mixed[:, :HEAD_DIM]), mixed[:, HEAD_DIM:])
    ).astype(bf16)
    delta = jnp.sum(grad * attention.astype(f32), axis=1, keepdims=True)
    prob_grad = dot_nt(packed_grad, key_values)
    score_grad = (probs * (prob_grad - delta) * scale).astype(bf16)
    mixed = dot(score_grad, key_values)
    query_grad = rope(
        reordered(jnp.where(first_half, mixed[:, :HEAD_DIM], turned(mixed[:, HEAD_DIM:]))), -1.0
    ).astype(bf16)
    key_value_grad = dot_tn(
        jnp.concatenate([score_grad, prob_weights], axis=0),
        jnp.concatenate([packed_query, packed_grad], axis=0),
    )
    kept[...] = key_value_grad[:, :HEAD_DIM]
    given[...] = key_value_grad[:, HEAD_DIM:].astype(bf16)
    low = joint[:, 2 * cols :]
    out_rank = low[:, 3 * ADAPTER_RANK : 4 * ADAPTER_RANK]
    for h in range(heads):
        lanes = slice(h * HEAD_DIM, (h + 1) * HEAD_DIM)
        of_head = attention[h * rows : (h + 1) * rows]
        riding[:, lanes] = query_grad[h * rows : (h + 1) * rows]
        attention_rows[:, lanes] = of_head
        riding[h * ADAPTER_RANK : (h + 1) * ADAPTER_RANK, cols : cols + HEAD_DIM] = dot_tn(
            out_rank, of_head
        ).astype(bf16)
    riding[:, cols + HEAD_DIM :] = low


def shards(
    hidden,
    upstream,
    query_frozen_weight,
    key_value_frozen_weight,
    output_frozen_weight,
    adapter_down,
    query_up_map,
    key_value_up_maps,
    output_down_map,
    output_up,
):
    ffn_count = lax.axis_size("ffn")
    width_count = lax.axis_size("width")
    ffn_index = lax.axis_index("ffn")
    width_index = lax.axis_index("width")
    parity = ffn_index % 2
    same_core = by_core(ffn_count)
    own_rows, width_cols = hidden.shape
    token_count = own_rows * ffn_count
    query_rows = token_count // width_count
    query_cols = query_frozen_weight.shape[1]
    key_cols = key_value_frozen_weight.shape[2]
    heads = query_cols // HEAD_DIM
    rank = ADAPTER_RANK
    score_scale = 1.0 / math.sqrt(HEAD_DIM)
    row_positions = width_index * query_rows + jnp.arange(query_rows, dtype=jnp.int32)

    query_weight = (
        query_frozen_weight.astype(f32) + adapter_scale * dot_tn(adapter_down[0], query_up_map)
    ).astype(bf16)
    key_value_weight = jnp.concatenate(
        [
            key_value_frozen_weight[k].astype(f32)
            + adapter_scale * dot_tn(adapter_down[k + 1], key_value_up_maps[k])
            for k in range(2)
        ],
        axis=1,
    ).astype(bf16)
    output_weight = (
        output_frozen_weight.astype(f32) + adapter_scale * dot_tn(output_down_map, output_up)
    ).astype(bf16)
    down = adapter_down.reshape(3 * rank, width_cols)
    low_weight = jnp.concatenate(
        [
            jnp.pad(down, ((0, HEAD_DIM - 3 * rank), (0, 0))),
            jnp.pad(output_up, ((3 * rank, HEAD_DIM - 4 * rank), (0, 0))),
        ],
        axis=1,
    ).T
    output_weight = output_weight.T
    query_tables = rope_tables(row_positions, 0, HEAD_DIM)
    key_tables = rope_tables(row_positions, ffn_index * key_cols, key_cols)
    input_weight = jnp.concatenate([query_weight, key_value_weight], axis=1)
    input_weight, query_tables, key_tables = lax.optimization_barrier(
        (input_weight, query_tables, key_tables)
    )

    both = jnp.concatenate([hidden, upstream], axis=1)
    own_core = sent_to_all(both, "ffn", same_core)
    own_core, low_weight, output_weight, key_value_weight, query_weight = lax.optimization_barrier(
        (own_core, low_weight, output_weight, key_value_weight, query_weight)
    )
    other_core = from_partner(own_core)
    rows = jnp.where(
        parity == 0,
        jnp.stack([own_core, other_core], axis=1),
        jnp.stack([other_core, own_core], axis=1),
    ).reshape(token_count, 2 * width_cols)
    hidden_rows = rows[:, :width_cols]
    upstream_rows = rows[:, width_cols:]

    place = jnp.stack([parity, width_index * query_rows]).astype(jnp.int32)
    smem = pl.BlockSpec(memory_space=pltpu.SMEM)
    vmem = pl.BlockSpec(memory_space=pltpu.VMEM)
    weights = (query_weight, output_weight, low_weight, key_value_weight)

    def of_blocks(blocks):
        return (
            jax.ShapeDtypeStruct((blocks, own_rows, 2 * query_cols + HEAD_DIM), bf16),
            jax.ShapeDtypeStruct((blocks, own_rows, 2 * key_cols), bf16),
        )

    cost = pl.CostEstimate(
        flops=token_count * width_cols * (2 * query_cols + 2 * HEAD_DIM),
        bytes_accessed=2**22,
        transcendentals=0,
    )
    own_parts = pl.pallas_call(
        own_projections,
        out_shape=of_blocks(ffn_count // 2),
        in_specs=[vmem] * 5,
        out_specs=(vmem, vmem),
        cost_estimate=cost,
        compiler_params=pltpu.CompilerParams(vmem_limit_bytes=20 * 2**20),
        name="own_projections",
    )(own_core, *weights)
    joint_part, key_value_part = pl.pallas_call(
        all_projections,
        out_shape=of_blocks(ffn_count),
        in_specs=[smem] + [vmem] * 7,
        out_specs=(vmem, vmem),
        cost_estimate=cost,
        compiler_params=pltpu.CompilerParams(vmem_limit_bytes=20 * 2**20),
        name="all_projections",
    )(place, other_core, *weights, *own_parts)
    joint_part = joint_part.reshape(token_count, -1)
    key_value_part = key_value_part.reshape(token_count, -1)
    joint_rows = lax.psum_scatter(joint_part, "width", scatter_dimension=0, tiled=True)

    key_value_sum = pieces_summed(key_value_part, "width")
    key_value_rows = jnp.concatenate(
        [rotate(key_value_sum[:, :key_cols], key_tables, 1.0), key_value_sum[:, key_cols:]], axis=1
    ).astype(bf16)
    own_half = lax.all_gather(key_value_rows, "width", axis=0, tiled=True)
    other_half = from_partner(own_half)

    riding, attention_rows, kept, given = pl.pallas_call(
        functools.partial(attention_block, heads=heads, scale=score_scale),
        out_shape=(
            jax.ShapeDtypeStruct((query_rows, query_cols + 2 * HEAD_DIM), bf16),
            jax.ShapeDtypeStruct((query_rows, query_cols), bf16),
            jax.ShapeDtypeStruct((token_count, 2 * key_cols), f32),
            jax.ShapeDtypeStruct((token_count, 2 * key_cols), bf16),
        ),
        in_specs=[smem] + [vmem] * 5,
        out_specs=(vmem,) * 4,
        cost_estimate=pl.CostEstimate(
            flops=12 * heads * query_rows * token_count * HEAD_DIM,
            bytes_accessed=2**21,
            transcendentals=heads * query_rows * token_count,
        ),
        compiler_params=pltpu.CompilerParams(vmem_limit_bytes=24 * 2**20),
        name="attention",
    )(place, joint_rows, own_half, other_half, *query_tables)
    query_grad = riding[:, :query_cols]

    gathered = lax.all_gather(riding, "width", axis=0, tiled=True)

    key_value_total = (kept + from_partner(given).astype(f32)).astype(bf16)
    terms = jnp.concatenate(
        [dot_nt(query_grad, query_up_map), dot_nt(attention_rows, output_down_map)], axis=1
    ).astype(bf16)
    key_value_total, terms = lax.optimization_barrier((key_value_total, terms))
    key_value_grad_sum = pieces_summed(key_value_total, "width")
    terms = lax.all_gather(terms, "ffn").astype(f32).sum(axis=0).astype(bf16)
    key_value_grad = jnp.concatenate(
        [
            rotate(key_value_grad_sum[:, :key_cols], key_tables, -1.0),
            key_value_grad_sum[:, key_cols:],
        ],
        axis=1,
    ).astype(bf16)
    key_value_gathered = lax.all_gather(
        jnp.concatenate([key_value_grad, terms], axis=1), "width", axis=0, tiled=True
    )
    key_value_grad_rows = key_value_gathered[:, : 2 * key_cols]
    key_value_terms = jnp.concatenate(
        [
            dot_nt(key_value_grad_rows[:, :key_cols], key_value_up_maps[0]),
            dot_nt(key_value_grad_rows[:, key_cols:], key_value_up_maps[1]),
        ],
        axis=1,
    ).astype(bf16)
    key_value_down = dot_tn(key_value_terms, hidden_rows)
    step = 1
    while step < 2:
        key_value_down = key_value_down + exchanged(key_value_down, step)
        step *= 2

    def input_part(of_core):
        def rows_of(values):
            by_owner = values.reshape(ffn_count // 2, 2, own_rows, -1)
            return lax.dynamic_index_in_dim(by_owner, of_core, 1, keepdims=False)

        grads = jnp.concatenate(
            [rows_of(gathered)[..., :query_cols], rows_of(key_value_grad_rows)], axis=-1
        ).reshape(ffn_count // 2 * own_rows, -1)
        return dot_nt(grads, input_weight)

    given = from_partner(input_part(1 - parity).astype(bf16))
    pair_sum = (input_part(parity) + given.astype(f32)).astype(bf16)
    pair_sum, key_value_down = lax.optimization_barrier((pair_sum, key_value_down))
    hidden_gradient = pieces_summed(pair_sum, "ffn", same_core).astype(bf16)
    while step < ffn_count:
        key_value_down = key_value_down + exchanged(key_value_down, step)
        step *= 2

    low = gathered[:, query_cols + HEAD_DIM :]
    query_rank = key_value_gathered[:, 2 * key_cols : 2 * key_cols + rank]
    outer_rank = key_value_gathered[:, 2 * key_cols + rank :]
    down_map_gradient = adapter_scale * jnp.concatenate(
        [dot_tn(query_rank, hidden_rows), key_value_down], axis=0
    ).reshape(adapter_down.shape)
    query_up_map_gradient = adapter_scale * dot_tn(low[:, :rank], gathered[:, :query_cols])
    key_value_up_maps_gradient = adapter_scale * jnp.stack(
        [
            dot_tn(low[:, rank : 2 * rank], key_value_grad_rows[:, :key_cols]),
            dot_tn(low[:, 2 * rank : 3 * rank], key_value_grad_rows[:, key_cols:]),
        ]
    )
    output_down_sum = (
        gathered[:, query_cols : query_cols + HEAD_DIM]
        .reshape(width_count, heads, rank, HEAD_DIM)
        .astype(f32)
        .sum(axis=0)
    )
    output_down_map_gradient = adapter_scale * output_down_sum.transpose(1, 0, 2).reshape(
        rank, query_cols
    )
    output_up_map_gradient = adapter_scale * dot_tn(outer_rank, upstream_rows)
    return (
        hidden_gradient,
        down_map_gradient,
        query_up_map_gradient,
        key_value_up_maps_gradient,
        output_down_map_gradient,
        output_up_map_gradient,
    )


def solution(mesh):
    placed = (
        P(("groups", "ffn"), "width"),
        P(("groups", "ffn"), "width"),
        P("width", "ffn"),
        P(None, "width", "ffn"),
        P("ffn", "width"),
        P("groups", None, "width"),
        P("groups", "ffn"),
        P("groups", None, "ffn"),
        P("groups", "ffn"),
        P("groups", "width"),
    )
    return jax.shard_map(
        shards,
        mesh=mesh,
        in_specs=placed,
        out_specs=(
            P(("groups", "ffn"), "width"),
            P("groups", None, "width"),
            P("groups", "ffn"),
            P("groups", None, "ffn"),
            P("groups", "ffn"),
            P("groups", "width"),
        ),
        check_vma=False,
    )
```

```python
import functools
import math

import jax
import jax.numpy as jnp
from jax import lax
from jax.experimental import pallas as pl
from jax.experimental.pallas import tpu as pltpu
from jax.sharding import PartitionSpec as P


HEAD_DIM = 128
ADAPTER_RANK = 16

adapter_scale = 2.0
rope_base = 500000.0

f32 = jnp.float32
bf16 = jnp.bfloat16


def dot(a, b):
    return jnp.dot(a, b, preferred_element_type=f32)


def dot_nt(a, b):
    return lax.dot_general(a, b, (((1,), (1,)), ((), ())), preferred_element_type=f32)


def dot_tn(a, b):
    return lax.dot_general(a, b, (((0,), (0,)), ((), ())), preferred_element_type=f32)


def by_core(size):
    return [[2 * k + c for k in range(size // 2)] for c in range(2)]


def exchanged(array, step):
    return lax.ppermute(array, "ffn", [(i, i ^ step) for i in range(lax.axis_size("ffn"))])


def from_partner(array):
    return exchanged(array, 1)


def sent_to_all(array, axis, groups=None):
    size = len(groups[0]) if groups else lax.axis_size(axis)
    copies = jnp.broadcast_to(array[None], (size, *array.shape))
    return lax.all_to_all(copies, axis, 0, 0, tiled=True, axis_index_groups=groups)


def pieces_summed(array, axis, groups=None):
    size = len(groups[0]) if groups else lax.axis_size(axis)
    pieces = array.reshape(size, array.shape[0] // size, *array.shape[1:])
    arrived = lax.all_to_all(pieces, axis, 0, 0, tiled=True, axis_index_groups=groups)
    return arrived.astype(f32).sum(axis=0)


def rope_tables(positions, first_dim, columns):
    dims = (first_dim + jnp.arange(columns, dtype=jnp.int32)) % HEAD_DIM
    pair_dims = dims - dims % 2
    frequency = jnp.exp(pair_dims.astype(f32) * (-math.log(rope_base) / HEAD_DIM))
    angles = positions.astype(f32)[:, None] * frequency[None, :]
    return jnp.cos(angles), jnp.sin(angles)


def rotate(values, tables, direction):
    cos, sin = tables
    is_even = jnp.arange(values.shape[-1], dtype=jnp.int32) % 2 == 0
    following = jnp.roll(values, -1, axis=-1)
    preceding = jnp.roll(values, 1, axis=-1)
    partner = jnp.where(is_even, -following, preceding)
    return values * cos + direction * partner * sin


def projected(part, query_weight, output_weight, low_weight, key_value_weight):
    chips, rows, both = part.shape
    tokens = part[...].reshape(chips * rows, both)
    hidden, upstream = tokens[:, : both // 2], tokens[:, both // 2 :]
    cols = query_weight.shape[1]
    end = cols + output_weight.shape[1]
    joint = (
        (dot(hidden, query_weight[...]).astype(bf16), slice(0, cols)),
        (dot(upstream, output_weight[...]).astype(bf16), slice(cols, end)),
        (dot(tokens, low_weight[...]).astype(bf16), slice(end, end + low_weight.shape[1])),
    )
    return joint, dot(hidden, key_value_weight[...]).astype(bf16)


def own_projections(
    own, query_weight, output_weight, low_weight, key_value_weight, joint, key_value
):
    values, of_key_value = projected(
        own, query_weight, output_weight, low_weight, key_value_weight
    )
    for value, lanes in values:
        joint[:, :, lanes] = value.reshape(*own.shape[:2], -1)
    key_value[...] = of_key_value.reshape(key_value.shape)


def all_projections(
    place,
    other,
    query_weight,
    output_weight,
    low_weight,
    key_value_weight,
    own_joint,
    own_key_value,
    joint,
    key_value,
):
    chips, rows, _ = other.shape
    values, of_key_value = projected(
        other, query_weight, output_weight, low_weight, key_value_weight
    )
    core = place[0]
    for chip in range(chips):
        here = slice(chip * rows, (chip + 1) * rows)
        joint[2 * chip + core] = own_joint[chip]
        key_value[2 * chip + core] = own_key_value[chip]
        for value, lanes in values:
            joint[2 * chip + 1 - core, :, lanes] = value[here]
        key_value[2 * chip + 1 - core] = of_key_value[here]


def attention_block(
    place, joint, own, other, cos, sin, riding, attention_rows, kept, given, *, heads, scale
):
    swapped = place[0] == 1
    rows = joint.shape[0]
    cols = heads * HEAD_DIM
    half = HEAD_DIM // 2

    def stacked(start):
        return jnp.concatenate(
            [joint[:, start + h * HEAD_DIM : start + (h + 1) * HEAD_DIM] for h in range(heads)],
            axis=0,
        ).astype(f32)

    def turned(values):
        return pltpu.roll(values, half, 1)

    def reordered(values):
        return jnp.where(swapped, turned(values), values)

    lane = lax.broadcasted_iota(jnp.int32, (heads * rows, HEAD_DIM), 1)
    first_half = lane < half
    is_even = lane % 2 == 0
    cosines = jnp.concatenate([cos[...]] * heads, axis=0)
    sines = jnp.concatenate([sin[...]] * heads, axis=0)

    def rope(values, direction):
        partner = jnp.where(
            is_even, -pltpu.roll(values, HEAD_DIM - 1, 1), pltpu.roll(values, 1, 1)
        )
        return values * cosines + direction * partner * sines

    query = reordered(rope(stacked(0), 1.0).astype(bf16).astype(f32))
    grad = stacked(cols)
    grad_own = reordered(grad)
    packed_query = jnp.concatenate(
        [jnp.where(first_half, query, 0.0), jnp.where(first_half, turned(query), 0.0)], axis=1
    ).astype(bf16)
    packed_grad = jnp.concatenate(
        [jnp.where(first_half, 0.0, turned(grad_own)), jnp.where(first_half, 0.0, grad_own)],
        axis=1,
    ).astype(bf16)
    key_values = jnp.concatenate([own[...], other[...]], axis=1)
    tokens = key_values.shape[0]
    scores = dot_nt(packed_query, key_values) * scale
    row = lax.broadcasted_iota(jnp.int32, (heads * rows, tokens), 0) % rows + place[1]
    causal = row >= lax.broadcasted_iota(jnp.int32, (heads * rows, tokens), 1)
    scores = jnp.where(causal, scores, -jnp.inf)
    shifted = jnp.exp(scores - jnp.max(scores, axis=1, keepdims=True))
    probs = shifted / jnp.sum(shifted, axis=1, keepdims=True)
    prob_weights = probs.astype(bf16)
    mixed = dot(prob_weights, key_values)
    attention = reordered(
        jnp.where(first_half, turned(mixed[:, :HEAD_DIM]), mixed[:, HEAD_DIM:])
    ).astype(bf16)
    delta = jnp.sum(grad * attention.astype(f32), axis=1, keepdims=True)
    prob_grad = dot_nt(packed_grad, key_values)
    score_grad = (probs * (prob_grad - delta) * scale).astype(bf16)
    mixed = dot(score_grad, key_values)
    query_grad = rope(
        reordered(jnp.where(first_half, mixed[:, :HEAD_DIM], turned(mixed[:, HEAD_DIM:]))), -1.0
    ).astype(bf16)
    key_value_grad = dot_tn(
        jnp.concatenate([score_grad, prob_weights], axis=0),
        jnp.concatenate([packed_query, packed_grad], axis=0),
    )
    kept[...] = key_value_grad[:, :HEAD_DIM]
    given[...] = key_value_grad[:, HEAD_DIM:].astype(bf16)
    low = joint[:, 2 * cols :]
    out_rank = low[:, 3 * ADAPTER_RANK : 4 * ADAPTER_RANK]
    for h in range(heads):
        lanes = slice(h * HEAD_DIM, (h + 1) * HEAD_DIM)
        of_head = attention[h * rows : (h + 1) * rows]
        riding[:, lanes] = query_grad[h * rows : (h + 1) * rows]
        attention_rows[:, lanes] = of_head
        riding[h * ADAPTER_RANK : (h + 1) * ADAPTER_RANK, cols : cols + HEAD_DIM] = dot_tn(
            out_rank, of_head
        ).astype(bf16)
    riding[:, cols + HEAD_DIM :] = low


def shards(
    hidden,
    upstream,
    query_frozen_weight,
    key_value_frozen_weight,
    output_frozen_weight,
    adapter_down,
    query_up_map,
    key_value_up_maps,
    output_down_map,
    output_up,
):
    ffn_count = lax.axis_size("ffn")
    width_count = lax.axis_size("width")
    ffn_index = lax.axis_index("ffn")
    width_index = lax.axis_index("width")
    parity = ffn_index % 2
    same_core = by_core(ffn_count)
    own_rows, width_cols = hidden.shape
    token_count = own_rows * ffn_count
    query_rows = token_count // width_count
    query_cols = query_frozen_weight.shape[1]
    key_cols = key_value_frozen_weight.shape[2]
    heads = query_cols // HEAD_DIM
    rank = ADAPTER_RANK
    score_scale = 1.0 / math.sqrt(HEAD_DIM)
    row_positions = width_index * query_rows + jnp.arange(query_rows, dtype=jnp.int32)

    query_weight = (
        query_frozen_weight.astype(f32) + adapter_scale * dot_tn(adapter_down[0], query_up_map)
    ).astype(bf16)
    key_value_weight = jnp.concatenate(
        [
            key_value_frozen_weight[k].astype(f32)
            + adapter_scale * dot_tn(adapter_down[k + 1], key_value_up_maps[k])
            for k in range(2)
        ],
        axis=1,
    ).astype(bf16)
    output_weight = (
        output_frozen_weight.astype(f32) + adapter_scale * dot_tn(output_down_map, output_up)
    ).astype(bf16)
    down = adapter_down.reshape(3 * rank, width_cols)
    low_weight = jnp.concatenate(
        [
            jnp.pad(down, ((0, HEAD_DIM - 3 * rank), (0, 0))),
            jnp.pad(output_up, ((3 * rank, HEAD_DIM - 4 * rank), (0, 0))),
        ],
        axis=1,
    ).T
    output_weight = output_weight.T
    query_tables = rope_tables(row_positions, 0, HEAD_DIM)
    key_tables = rope_tables(row_positions, ffn_index * key_cols, key_cols)
    input_weight = jnp.concatenate([query_weight, key_value_weight], axis=1)
    input_weight, query_tables, key_tables = lax.optimization_barrier(
        (input_weight, query_tables, key_tables)
    )

    both = jnp.concatenate([hidden, upstream], axis=1)
    own_core = sent_to_all(both, "ffn", same_core)
    own_core, low_weight, output_weight, key_value_weight, query_weight = lax.optimization_barrier(
        (own_core, low_weight, output_weight, key_value_weight, query_weight)
    )
    other_core = from_partner(own_core)
    rows = jnp.where(
        parity == 0,
        jnp.stack([own_core, other_core], axis=1),
        jnp.stack([other_core, own_core], axis=1),
    ).reshape(token_count, 2 * width_cols)
    hidden_rows = rows[:, :width_cols]
    upstream_rows = rows[:, width_cols:]

    place = jnp.stack([parity, width_index * query_rows]).astype(jnp.int32)
    smem = pl.BlockSpec(memory_space=pltpu.SMEM)
    vmem = pl.BlockSpec(memory_space=pltpu.VMEM)
    weights = (query_weight, output_weight, low_weight, key_value_weight)

    def of_blocks(blocks):
        return (
            jax.ShapeDtypeStruct((blocks, own_rows, 2 * query_cols + HEAD_DIM), bf16),
            jax.ShapeDtypeStruct((blocks, own_rows, 2 * key_cols), bf16),
        )

    cost = pl.CostEstimate(
        flops=token_count * width_cols * (2 * query_cols + 2 * HEAD_DIM),
        bytes_accessed=2**22,
        transcendentals=0,
    )
    own_parts = pl.pallas_call(
        own_projections,
        out_shape=of_blocks(ffn_count // 2),
        in_specs=[vmem] * 5,
        out_specs=(vmem, vmem),
        cost_estimate=cost,
        compiler_params=pltpu.CompilerParams(vmem_limit_bytes=20 * 2**20),
        name="own_projections",
    )(own_core, *weights)
    joint_part, key_value_part = pl.pallas_call(
        all_projections,
        out_shape=of_blocks(ffn_count),
        in_specs=[smem] + [vmem] * 7,
        out_specs=(vmem, vmem),
        cost_estimate=cost,
        compiler_params=pltpu.CompilerParams(vmem_limit_bytes=20 * 2**20),
        name="all_projections",
    )(place, other_core, *weights, *own_parts)
    joint_part = joint_part.reshape(token_count, -1)
    key_value_part = key_value_part.reshape(token_count, -1)
    joint_rows = lax.psum_scatter(joint_part, "width", scatter_dimension=0, tiled=True)

    key_value_sum = pieces_summed(key_value_part, "width")
    key_value_rows = jnp.concatenate(
        [rotate(key_value_sum[:, :key_cols], key_tables, 1.0), key_value_sum[:, key_cols:]], axis=1
    ).astype(bf16)
    own_half = lax.all_gather(key_value_rows, "width", axis=0, tiled=True)
    other_half = from_partner(own_half)

    riding, attention_rows, kept, given = pl.pallas_call(
        functools.partial(attention_block, heads=heads, scale=score_scale),
        out_shape=(
            jax.ShapeDtypeStruct((query_rows, query_cols + 2 * HEAD_DIM), bf16),
            jax.ShapeDtypeStruct((query_rows, query_cols), bf16),
            jax.ShapeDtypeStruct((token_count, 2 * key_cols), f32),
            jax.ShapeDtypeStruct((token_count, 2 * key_cols), bf16),
        ),
        in_specs=[smem] + [vmem] * 5,
        out_specs=(vmem,) * 4,
        cost_estimate=pl.CostEstimate(
            flops=12 * heads * query_rows * token_count * HEAD_DIM,
            bytes_accessed=2**21,
            transcendentals=heads * query_rows * token_count,
        ),
        compiler_params=pltpu.CompilerParams(vmem_limit_bytes=24 * 2**20),
        name="attention",
    )(place, joint_rows, own_half, other_half, *query_tables)
    query_grad = riding[:, :query_cols]

    gathered = lax.all_gather(riding, "width", axis=0, tiled=True)

    key_value_total = (kept + from_partner(given).astype(f32)).astype(bf16)
    terms = jnp.concatenate(
        [dot_nt(query_grad, query_up_map), dot_nt(attention_rows, output_down_map)], axis=1
    ).astype(bf16)
    key_value_total, terms = lax.optimization_barrier((key_value_total, terms))
    key_value_grad_sum = pieces_summed(key_value_total, "width")
    terms = lax.all_gather(terms, "ffn").astype(f32).sum(axis=0).astype(bf16)
    key_value_grad = jnp.concatenate(
        [
            rotate(key_value_grad_sum[:, :key_cols], key_tables, -1.0),
            key_value_grad_sum[:, key_cols:],
        ],
        axis=1,
    ).astype(bf16)
    key_value_gathered = lax.all_gather(
        jnp.concatenate([key_value_grad, terms], axis=1), "width", axis=0, tiled=True
    )
    key_value_grad_rows = key_value_gathered[:, : 2 * key_cols]
    key_value_terms = jnp.concatenate(
        [
            dot_nt(key_value_grad_rows[:, :key_cols], key_value_up_maps[0]),
            dot_nt(key_value_grad_rows[:, key_cols:], key_value_up_maps[1]),
        ],
        axis=1,
    ).astype(bf16)
    key_value_down = dot_tn(key_value_terms, hidden_rows)
    key_value_down = (key_value_down + from_partner(key_value_down)).astype(bf16)
    key_value_down = sent_to_all(key_value_down, "ffn", same_core)

    def input_part(of_core):
        def rows_of(values):
            by_owner = values.reshape(ffn_count // 2, 2, own_rows, -1)
            return lax.dynamic_index_in_dim(by_owner, of_core, 1, keepdims=False)

        grads = jnp.concatenate(
            [rows_of(gathered)[..., :query_cols], rows_of(key_value_grad_rows)], axis=-1
        ).reshape(ffn_count // 2 * own_rows, -1)
        return dot_nt(grads, input_weight)

    given = from_partner(input_part(1 - parity).astype(bf16))
    given, key_value_down = lax.optimization_barrier((given, key_value_down))
    pair_sum = (input_part(parity) + given.astype(f32)).astype(bf16)
    hidden_gradient = pieces_summed(pair_sum, "ffn", same_core).astype(bf16)
    key_value_down = key_value_down.astype(f32).sum(axis=0)

    low = gathered[:, query_cols + HEAD_DIM :]
    query_rank = key_value_gathered[:, 2 * key_cols : 2 * key_cols + rank]
    outer_rank = key_value_gathered[:, 2 * key_cols + rank :]
    down_map_gradient = adapter_scale * jnp.concatenate(
        [dot_tn(query_rank, hidden_rows), key_value_down], axis=0
    ).reshape(adapter_down.shape)
    query_up_map_gradient = adapter_scale * dot_tn(low[:, :rank], gathered[:, :query_cols])
    key_value_up_maps_gradient = adapter_scale * jnp.stack(
        [
            dot_tn(low[:, rank : 2 * rank], key_value_grad_rows[:, :key_cols]),
            dot_tn(low[:, 2 * rank : 3 * rank], key_value_grad_rows[:, key_cols:]),
        ]
    )
    output_down_sum = (
        gathered[:, query_cols : query_cols + HEAD_DIM]
        .reshape(width_count, heads, rank, HEAD_DIM)
        .astype(f32)
        .sum(axis=0)
    )
    output_down_map_gradient = adapter_scale * output_down_sum.transpose(1, 0, 2).reshape(
        rank, query_cols
    )
    output_up_map_gradient = adapter_scale * dot_tn(outer_rank, upstream_rows)
    return (
        hidden_gradient,
        down_map_gradient,
        query_up_map_gradient,
        key_value_up_maps_gradient,
        output_down_map_gradient,
        output_up_map_gradient,
    )


def solution(mesh):
    placed = (
        P(("groups", "ffn"), "width"),
        P(("groups", "ffn"), "width"),
        P("width", "ffn"),
        P(None, "width", "ffn"),
        P("ffn", "width"),
        P("groups", None, "width"),
        P("groups", "ffn"),
        P("groups", None, "ffn"),
        P("groups", "ffn"),
        P("groups", "width"),
    )
    return jax.shard_map(
        shards,
        mesh=mesh,
        in_specs=placed,
        out_specs=(
            P(("groups", "ffn"), "width"),
            P("groups", None, "width"),
            P("groups", "ffn"),
            P("groups", None, "ffn"),
            P("groups", "ffn"),
            P("groups", "width"),
        ),
        check_vma=False,
    )
```

```python
import functools
import math

import jax
import jax.numpy as jnp
from jax import lax
from jax.experimental import pallas as pl
from jax.experimental.pallas import tpu as pltpu
from jax.sharding import PartitionSpec as P


HEAD_DIM = 128
ADAPTER_RANK = 16

adapter_scale = 2.0
rope_base = 500000.0

f32 = jnp.float32
bf16 = jnp.bfloat16


def dot(a, b):
    return jnp.dot(a, b, preferred_element_type=f32)


def dot_nt(a, b):
    return lax.dot_general(a, b, (((1,), (1,)), ((), ())), preferred_element_type=f32)


def dot_tn(a, b):
    return lax.dot_general(a, b, (((0,), (0,)), ((), ())), preferred_element_type=f32)


def by_core(size):
    return [[2 * k + c for k in range(size // 2)] for c in range(2)]


def exchanged(array, step):
    return lax.ppermute(array, "ffn", [(i, i ^ step) for i in range(lax.axis_size("ffn"))])


def from_partner(array):
    return exchanged(array, 1)


def sent_to_all(array, axis, groups=None):
    size = len(groups[0]) if groups else lax.axis_size(axis)
    copies = jnp.broadcast_to(array[None], (size, *array.shape))
    return lax.all_to_all(copies, axis, 0, 0, tiled=True, axis_index_groups=groups)


def pieces_summed(array, axis, groups=None):
    size = len(groups[0]) if groups else lax.axis_size(axis)
    pieces = array.reshape(size, array.shape[0] // size, *array.shape[1:])
    arrived = lax.all_to_all(pieces, axis, 0, 0, tiled=True, axis_index_groups=groups)
    return arrived.astype(f32).sum(axis=0)


def rope_tables(positions, first_dim, columns):
    dims = (first_dim + jnp.arange(columns, dtype=jnp.int32)) % HEAD_DIM
    pair_dims = dims - dims % 2
    frequency = jnp.exp(pair_dims.astype(f32) * (-math.log(rope_base) / HEAD_DIM))
    angles = positions.astype(f32)[:, None] * frequency[None, :]
    return jnp.cos(angles), jnp.sin(angles)


def rotate(values, tables, direction):
    cos, sin = tables
    is_even = jnp.arange(values.shape[-1], dtype=jnp.int32) % 2 == 0
    following = jnp.roll(values, -1, axis=-1)
    preceding = jnp.roll(values, 1, axis=-1)
    partner = jnp.where(is_even, -following, preceding)
    return values * cos + direction * partner * sin


def projected(part, query_weight, output_weight, low_weight, key_value_weight):
    chips, rows, both = part.shape
    tokens = part[...].reshape(chips * rows, both)
    hidden, upstream = tokens[:, : both // 2], tokens[:, both // 2 :]
    cols = query_weight.shape[1]
    end = cols + output_weight.shape[1]
    joint = (
        (dot(hidden, query_weight[...]).astype(bf16), slice(0, cols)),
        (dot(upstream, output_weight[...]).astype(bf16), slice(cols, end)),
        (dot(tokens, low_weight[...]).astype(bf16), slice(end, end + low_weight.shape[1])),
    )
    return joint, dot(hidden, key_value_weight[...]).astype(bf16)


def own_projections(
    own, query_weight, output_weight, low_weight, key_value_weight, joint, key_value
):
    values, of_key_value = projected(
        own, query_weight, output_weight, low_weight, key_value_weight
    )
    for value, lanes in values:
        joint[:, :, lanes] = value.reshape(*own.shape[:2], -1)
    key_value[...] = of_key_value.reshape(key_value.shape)


def all_projections(
    place,
    other,
    query_weight,
    output_weight,
    low_weight,
    key_value_weight,
    own_joint,
    own_key_value,
    joint,
    key_value,
):
    chips, rows, _ = other.shape
    values, of_key_value = projected(
        other, query_weight, output_weight, low_weight, key_value_weight
    )
    core = place[0]
    for chip in range(chips):
        here = slice(chip * rows, (chip + 1) * rows)
        joint[2 * chip + core] = own_joint[chip]
        key_value[2 * chip + core] = own_key_value[chip]
        for value, lanes in values:
            joint[2 * chip + 1 - core, :, lanes] = value[here]
        key_value[2 * chip + 1 - core] = of_key_value[here]


def input_parts(place, query_grad, key_value_grad, weight, given, kept):
    cols = weight.shape[0] - key_value_grad.shape[2]
    chips = query_grad.shape[0] // 2
    for out, core in ((given, 1 - place[0]), (kept, place[0])):
        blocks = [
            jnp.concatenate(
                [query_grad[2 * chip + core, :, :cols], key_value_grad[2 * chip + core]], axis=1
            )
            for chip in range(chips)
        ]
        out[...] = dot(jnp.concatenate(blocks, axis=0), weight[...]).astype(out.dtype)


def attention_block(
    place, joint, own, other, cos, sin, riding, attention_rows, kept, given, *, heads, scale
):
    swapped = place[0] == 1
    rows = joint.shape[0]
    cols = heads * HEAD_DIM
    half = HEAD_DIM // 2

    def stacked(start):
        return jnp.concatenate(
            [joint[:, start + h * HEAD_DIM : start + (h + 1) * HEAD_DIM] for h in range(heads)],
            axis=0,
        ).astype(f32)

    def turned(values):
        return pltpu.roll(values, half, 1)

    def reordered(values):
        return jnp.where(swapped, turned(values), values)

    lane = lax.broadcasted_iota(jnp.int32, (heads * rows, HEAD_DIM), 1)
    first_half = lane < half
    is_even = lane % 2 == 0
    cosines = jnp.concatenate([cos[...]] * heads, axis=0)
    sines = jnp.concatenate([sin[...]] * heads, axis=0)

    def rope(values, direction):
        partner = jnp.where(
            is_even, -pltpu.roll(values, HEAD_DIM - 1, 1), pltpu.roll(values, 1, 1)
        )
        return values * cosines + direction * partner * sines

    query = reordered(rope(stacked(0), 1.0).astype(bf16).astype(f32))
    grad = stacked(cols)
    grad_own = reordered(grad)
    packed_query = jnp.concatenate(
        [jnp.where(first_half, query, 0.0), jnp.where(first_half, turned(query), 0.0)], axis=1
    ).astype(bf16)
    packed_grad = jnp.concatenate(
        [jnp.where(first_half, 0.0, turned(grad_own)), jnp.where(first_half, 0.0, grad_own)],
        axis=1,
    ).astype(bf16)
    key_values = jnp.concatenate([own[...], other[...]], axis=1)
    tokens = key_values.shape[0]
    scores = dot_nt(packed_query, key_values) * scale
    row = lax.broadcasted_iota(jnp.int32, (heads * rows, tokens), 0) % rows + place[1]
    causal = row >= lax.broadcasted_iota(jnp.int32, (heads * rows, tokens), 1)
    scores = jnp.where(causal, scores, -jnp.inf)
    shifted = jnp.exp(scores - jnp.max(scores, axis=1, keepdims=True))
    probs = shifted / jnp.sum(shifted, axis=1, keepdims=True)
    prob_weights = probs.astype(bf16)
    mixed = dot(prob_weights, key_values)
    attention = reordered(
        jnp.where(first_half, turned(mixed[:, :HEAD_DIM]), mixed[:, HEAD_DIM:])
    ).astype(bf16)
    delta = jnp.sum(grad * attention.astype(f32), axis=1, keepdims=True)
    prob_grad = dot_nt(packed_grad, key_values)
    score_grad = (probs * (prob_grad - delta) * scale).astype(bf16)
    mixed = dot(score_grad, key_values)
    query_grad = rope(
        reordered(jnp.where(first_half, mixed[:, :HEAD_DIM], turned(mixed[:, HEAD_DIM:]))), -1.0
    ).astype(bf16)
    key_value_grad = dot_tn(
        jnp.concatenate([score_grad, prob_weights], axis=0),
        jnp.concatenate([packed_query, packed_grad], axis=0),
    )
    kept[...] = key_value_grad[:, :HEAD_DIM]
    given[...] = key_value_grad[:, HEAD_DIM:].astype(bf16)
    low = joint[:, 2 * cols :]
    out_rank = low[:, 3 * ADAPTER_RANK : 4 * ADAPTER_RANK]
    for h in range(heads):
        lanes = slice(h * HEAD_DIM, (h + 1) * HEAD_DIM)
        of_head = attention[h * rows : (h + 1) * rows]
        riding[:, lanes] = query_grad[h * rows : (h + 1) * rows]
        attention_rows[:, lanes] = of_head
        riding[h * ADAPTER_RANK : (h + 1) * ADAPTER_RANK, cols : cols + HEAD_DIM] = dot_tn(
            out_rank, of_head
        ).astype(bf16)
    riding[:, cols + HEAD_DIM :] = low


def shards(
    hidden,
    upstream,
    query_frozen_weight,
    key_value_frozen_weight,
    output_frozen_weight,
    adapter_down,
    query_up_map,
    key_value_up_maps,
    output_down_map,
    output_up,
):
    ffn_count = lax.axis_size("ffn")
    width_count = lax.axis_size("width")
    ffn_index = lax.axis_index("ffn")
    width_index = lax.axis_index("width")
    parity = ffn_index % 2
    same_core = by_core(ffn_count)
    own_rows, width_cols = hidden.shape
    token_count = own_rows * ffn_count
    query_rows = token_count // width_count
    query_cols = query_frozen_weight.shape[1]
    key_cols = key_value_frozen_weight.shape[2]
    heads = query_cols // HEAD_DIM
    rank = ADAPTER_RANK
    score_scale = 1.0 / math.sqrt(HEAD_DIM)
    row_positions = width_index * query_rows + jnp.arange(query_rows, dtype=jnp.int32)

    query_weight = (
        query_frozen_weight.astype(f32) + adapter_scale * dot_tn(adapter_down[0], query_up_map)
    ).astype(bf16)
    key_value_weight = jnp.concatenate(
        [
            key_value_frozen_weight[k].astype(f32)
            + adapter_scale * dot_tn(adapter_down[k + 1], key_value_up_maps[k])
            for k in range(2)
        ],
        axis=1,
    ).astype(bf16)
    output_weight = (
        output_frozen_weight.astype(f32) + adapter_scale * dot_tn(output_down_map, output_up)
    ).astype(bf16)
    down = adapter_down.reshape(3 * rank, width_cols)
    low_weight = jnp.concatenate(
        [
            jnp.pad(down, ((0, HEAD_DIM - 3 * rank), (0, 0))),
            jnp.pad(output_up, ((3 * rank, HEAD_DIM - 4 * rank), (0, 0))),
        ],
        axis=1,
    ).T
    output_weight = output_weight.T
    query_tables = rope_tables(row_positions, 0, HEAD_DIM)
    key_tables = rope_tables(row_positions, ffn_index * key_cols, key_cols)
    input_weight = jnp.concatenate([query_weight, key_value_weight], axis=1).T
    input_weight, query_tables, key_tables = lax.optimization_barrier(
        (input_weight, query_tables, key_tables)
    )

    both = jnp.concatenate([hidden, upstream], axis=1)
    own_core = sent_to_all(both, "ffn", same_core)
    own_core, low_weight, output_weight, key_value_weight, query_weight = lax.optimization_barrier(
        (own_core, low_weight, output_weight, key_value_weight, query_weight)
    )
    other_core = from_partner(own_core)
    rows = jnp.where(
        parity == 0,
        jnp.stack([own_core, other_core], axis=1),
        jnp.stack([other_core, own_core], axis=1),
    ).reshape(token_count, 2 * width_cols)
    hidden_rows = rows[:, :width_cols]
    upstream_rows = rows[:, width_cols:]

    place = jnp.stack([parity, width_index * query_rows]).astype(jnp.int32)
    smem = pl.BlockSpec(memory_space=pltpu.SMEM)
    vmem = pl.BlockSpec(memory_space=pltpu.VMEM)
    weights = (query_weight, output_weight, low_weight, key_value_weight)

    def of_blocks(blocks):
        return (
            jax.ShapeDtypeStruct((blocks, own_rows, 2 * query_cols + HEAD_DIM), bf16),
            jax.ShapeDtypeStruct((blocks, own_rows, 2 * key_cols), bf16),
        )

    cost = pl.CostEstimate(
        flops=token_count * width_cols * (2 * query_cols + 2 * HEAD_DIM),
        bytes_accessed=2**22,
        transcendentals=0,
    )
    own_parts = pl.pallas_call(
        own_projections,
        out_shape=of_blocks(ffn_count // 2),
        in_specs=[vmem] * 5,
        out_specs=(vmem, vmem),
        cost_estimate=cost,
        compiler_params=pltpu.CompilerParams(vmem_limit_bytes=20 * 2**20),
        name="own_projections",
    )(own_core, *weights)
    joint_part, key_value_part = pl.pallas_call(
        all_projections,
        out_shape=of_blocks(ffn_count),
        in_specs=[smem] + [vmem] * 7,
        out_specs=(vmem, vmem),
        cost_estimate=cost,
        compiler_params=pltpu.CompilerParams(vmem_limit_bytes=20 * 2**20),
        name="all_projections",
    )(place, other_core, *weights, *own_parts)
    joint_part = joint_part.reshape(token_count, -1)
    key_value_part = key_value_part.reshape(token_count, -1)
    joint_rows = lax.psum_scatter(joint_part, "width", scatter_dimension=0, tiled=True)

    key_value_sum = pieces_summed(key_value_part, "width")
    key_value_rows = jnp.concatenate(
        [rotate(key_value_sum[:, :key_cols], key_tables, 1.0), key_value_sum[:, key_cols:]], axis=1
    ).astype(bf16)
    own_half = lax.all_gather(key_value_rows, "width", axis=0, tiled=True)
    other_half = from_partner(own_half)

    riding, attention_rows, kept, given = pl.pallas_call(
        functools.partial(attention_block, heads=heads, scale=score_scale),
        out_shape=(
            jax.ShapeDtypeStruct((query_rows, query_cols + 2 * HEAD_DIM), bf16),
            jax.ShapeDtypeStruct((query_rows, query_cols), bf16),
            jax.ShapeDtypeStruct((token_count, 2 * key_cols), f32),
            jax.ShapeDtypeStruct((token_count, 2 * key_cols), bf16),
        ),
        in_specs=[smem] + [vmem] * 5,
        out_specs=(vmem,) * 4,
        cost_estimate=pl.CostEstimate(
            flops=12 * heads * query_rows * token_count * HEAD_DIM,
            bytes_accessed=2**21,
            transcendentals=heads * query_rows * token_count,
        ),
        compiler_params=pltpu.CompilerParams(vmem_limit_bytes=24 * 2**20),
        name="attention",
    )(place, joint_rows, own_half, other_half, *query_tables)
    query_grad = riding[:, :query_cols]

    gathered = lax.all_gather(riding, "width", axis=0, tiled=True)

    key_value_total = (kept + from_partner(given).astype(f32)).astype(bf16)
    terms = jnp.concatenate(
        [dot_nt(query_grad, query_up_map), dot_nt(attention_rows, output_down_map)], axis=1
    ).astype(bf16)
    key_value_total, terms = lax.optimization_barrier((key_value_total, terms))
    key_value_grad_sum = pieces_summed(key_value_total, "width")
    terms = lax.all_gather(terms, "ffn").astype(f32).sum(axis=0).astype(bf16)
    key_value_grad = jnp.concatenate(
        [
            rotate(key_value_grad_sum[:, :key_cols], key_tables, -1.0),
            key_value_grad_sum[:, key_cols:],
        ],
        axis=1,
    ).astype(bf16)
    key_value_gathered = lax.all_gather(
        jnp.concatenate([key_value_grad, terms], axis=1), "width", axis=0, tiled=True
    )
    key_value_grad_rows = key_value_gathered[:, : 2 * key_cols]
    key_value_terms = jnp.concatenate(
        [
            dot_nt(key_value_grad_rows[:, :key_cols], key_value_up_maps[0]),
            dot_nt(key_value_grad_rows[:, key_cols:], key_value_up_maps[1]),
        ],
        axis=1,
    ).astype(bf16)
    key_value_down = dot_tn(key_value_terms, hidden_rows)
    key_value_down = sent_to_all(key_value_down.astype(bf16), "ffn", same_core)

    given, kept = pl.pallas_call(
        input_parts,
        out_shape=(
            jax.ShapeDtypeStruct((token_count // 2, width_cols), bf16),
            jax.ShapeDtypeStruct((token_count // 2, width_cols), f32),
        ),
        in_specs=[smem] + [vmem] * 3,
        out_specs=(vmem, vmem),
        cost_estimate=pl.CostEstimate(
            flops=2 * token_count * width_cols * input_weight.shape[0],
            bytes_accessed=2**22,
            transcendentals=0,
        ),
        compiler_params=pltpu.CompilerParams(vmem_limit_bytes=20 * 2**20),
        name="input_parts",
    )(
        place,
        gathered.reshape(ffn_count, own_rows, -1),
        key_value_grad_rows.reshape(ffn_count, own_rows, -1),
        input_weight,
    )
    given = from_partner(given)
    given, key_value_down = lax.optimization_barrier((given, key_value_down))
    pair_sum = (kept + given.astype(f32)).astype(bf16)
    hidden_gradient = pieces_summed(pair_sum, "ffn", same_core).astype(bf16)
    key_value_down = key_value_down.astype(f32).sum(axis=0)
    key_value_down = key_value_down + from_partner(key_value_down)

    low = gathered[:, query_cols + HEAD_DIM :]
    query_rank = key_value_gathered[:, 2 * key_cols : 2 * key_cols + rank]
    outer_rank = key_value_gathered[:, 2 * key_cols + rank :]
    down_map_gradient = adapter_scale * jnp.concatenate(
        [dot_tn(query_rank, hidden_rows), key_value_down], axis=0
    ).reshape(adapter_down.shape)
    query_up_map_gradient = adapter_scale * dot_tn(low[:, :rank], gathered[:, :query_cols])
    key_value_up_maps_gradient = adapter_scale * jnp.stack(
        [
            dot_tn(low[:, rank : 2 * rank], key_value_grad_rows[:, :key_cols]),
            dot_tn(low[:, 2 * rank : 3 * rank], key_value_grad_rows[:, key_cols:]),
        ]
    )
    output_down_sum = (
        gathered[:, query_cols : query_cols + HEAD_DIM]
        .reshape(width_count, heads, rank, HEAD_DIM)
        .astype(f32)
        .sum(axis=0)
    )
    output_down_map_gradient = adapter_scale * output_down_sum.transpose(1, 0, 2).reshape(
        rank, query_cols
    )
    output_up_map_gradient = adapter_scale * dot_tn(outer_rank, upstream_rows)
    return (
        hidden_gradient,
        down_map_gradient,
        query_up_map_gradient,
        key_value_up_maps_gradient,
        output_down_map_gradient,
        output_up_map_gradient,
    )


def solution(mesh):
    placed = (
        P(("groups", "ffn"), "width"),
        P(("groups", "ffn"), "width"),
        P("width", "ffn"),
        P(None, "width", "ffn"),
        P("ffn", "width"),
        P("groups", None, "width"),
        P("groups", "ffn"),
        P("groups", None, "ffn"),
        P("groups", "ffn"),
        P("groups", "width"),
    )
    return jax.shard_map(
        shards,
        mesh=mesh,
        in_specs=placed,
        out_specs=(
            P(("groups", "ffn"), "width"),
            P("groups", None, "width"),
            P("groups", "ffn"),
            P("groups", None, "ffn"),
            P("groups", "ffn"),
            P("groups", "width"),
        ),
        check_vma=False,
    )
```

```python
import functools
import math

import jax
import jax.numpy as jnp
from jax import lax
from jax.experimental import pallas as pl
from jax.experimental.pallas import tpu as pltpu
from jax.sharding import PartitionSpec as P


HEAD_DIM = 128
ADAPTER_RANK = 16

adapter_scale = 2.0
rope_base = 500000.0

f32 = jnp.float32
bf16 = jnp.bfloat16


def dot(a, b):
    return jnp.dot(a, b, preferred_element_type=f32)


def dot_nt(a, b):
    return lax.dot_general(a, b, (((1,), (1,)), ((), ())), preferred_element_type=f32)


def dot_tn(a, b):
    return lax.dot_general(a, b, (((0,), (0,)), ((), ())), preferred_element_type=f32)


def by_core(size):
    return [[2 * k + c for k in range(size // 2)] for c in range(2)]


def exchanged(array, step):
    return lax.ppermute(array, "ffn", [(i, i ^ step) for i in range(lax.axis_size("ffn"))])


def from_partner(array):
    return exchanged(array, 1)


def sent_to_all(array, axis, groups=None):
    size = len(groups[0]) if groups else lax.axis_size(axis)
    copies = jnp.broadcast_to(array[None], (size, *array.shape))
    return lax.all_to_all(copies, axis, 0, 0, tiled=True, axis_index_groups=groups)


def pieces_summed(array, axis, groups=None):
    size = len(groups[0]) if groups else lax.axis_size(axis)
    pieces = array.reshape(size, array.shape[0] // size, *array.shape[1:])
    arrived = lax.all_to_all(pieces, axis, 0, 0, tiled=True, axis_index_groups=groups)
    return arrived.astype(f32).sum(axis=0)


def rope_tables(positions, first_dim, columns):
    dims = (first_dim + jnp.arange(columns, dtype=jnp.int32)) % HEAD_DIM
    pair_dims = dims - dims % 2
    frequency = jnp.exp(pair_dims.astype(f32) * (-math.log(rope_base) / HEAD_DIM))
    angles = positions.astype(f32)[:, None] * frequency[None, :]
    return jnp.cos(angles), jnp.sin(angles)


def rotate(values, tables, direction):
    cos, sin = tables
    is_even = jnp.arange(values.shape[-1], dtype=jnp.int32) % 2 == 0
    following = jnp.roll(values, -1, axis=-1)
    preceding = jnp.roll(values, 1, axis=-1)
    partner = jnp.where(is_even, -following, preceding)
    return values * cos + direction * partner * sin


def projected(part, query_weight, output_weight, low_weight, key_value_weight):
    chips, rows, both = part.shape
    tokens = part[...].reshape(chips * rows, both)
    hidden, upstream = tokens[:, : both // 2], tokens[:, both // 2 :]
    cols = query_weight.shape[1]
    end = cols + output_weight.shape[1]
    joint = (
        (dot(hidden, query_weight[...]).astype(bf16), slice(0, cols)),
        (dot(upstream, output_weight[...]).astype(bf16), slice(cols, end)),
        (dot(tokens, low_weight[...]).astype(bf16), slice(end, end + low_weight.shape[1])),
    )
    return joint, dot(hidden, key_value_weight[...]).astype(bf16)


def own_projections(
    own, query_weight, output_weight, low_weight, key_value_weight, joint, key_value
):
    values, of_key_value = projected(
        own, query_weight, output_weight, low_weight, key_value_weight
    )
    for value, lanes in values:
        joint[:, :, lanes] = value.reshape(*own.shape[:2], -1)
    key_value[...] = of_key_value.reshape(key_value.shape)


def all_projections(
    place,
    other,
    query_weight,
    output_weight,
    low_weight,
    key_value_weight,
    own_joint,
    own_key_value,
    joint,
    key_value,
):
    chips, rows, _ = other.shape
    values, of_key_value = projected(
        other, query_weight, output_weight, low_weight, key_value_weight
    )
    core = place[0]
    for chip in range(chips):
        here = slice(chip * rows, (chip + 1) * rows)
        joint[2 * chip + core] = own_joint[chip]
        key_value[2 * chip + core] = own_key_value[chip]
        for value, lanes in values:
            joint[2 * chip + 1 - core, :, lanes] = value[here]
        key_value[2 * chip + 1 - core] = of_key_value[here]


def input_parts(place, query_grad, key_value_grad, weight, given, kept):
    cols = weight.shape[0] - key_value_grad.shape[2]
    chips = query_grad.shape[0] // 2
    for out, core in ((given, 1 - place[0]), (kept, place[0])):
        blocks = [
            jnp.concatenate(
                [query_grad[2 * chip + core, :, :cols], key_value_grad[2 * chip + core]], axis=1
            )
            for chip in range(chips)
        ]
        out[...] = dot(jnp.concatenate(blocks, axis=0), weight[...]).astype(out.dtype)


def attention_block(
    place, joint, own, other, cos, sin, riding, attention_rows, kept, given, *, heads, scale
):
    swapped = place[0] == 1
    rows = joint.shape[0]
    cols = heads * HEAD_DIM
    half = HEAD_DIM // 2

    def stacked(start):
        return jnp.concatenate(
            [joint[:, start + h * HEAD_DIM : start + (h + 1) * HEAD_DIM] for h in range(heads)],
            axis=0,
        ).astype(f32)

    def turned(values):
        return pltpu.roll(values, half, 1)

    def reordered(values):
        return jnp.where(swapped, turned(values), values)

    lane = lax.broadcasted_iota(jnp.int32, (heads * rows, HEAD_DIM), 1)
    first_half = lane < half
    is_even = lane % 2 == 0
    cosines = jnp.concatenate([cos[...]] * heads, axis=0)
    sines = jnp.concatenate([sin[...]] * heads, axis=0)

    def rope(values, direction):
        partner = jnp.where(
            is_even, -pltpu.roll(values, HEAD_DIM - 1, 1), pltpu.roll(values, 1, 1)
        )
        return values * cosines + direction * partner * sines

    query = reordered(rope(stacked(0), 1.0).astype(bf16).astype(f32))
    grad = stacked(cols)
    grad_own = reordered(grad)
    packed_query = jnp.concatenate(
        [jnp.where(first_half, query, 0.0), jnp.where(first_half, turned(query), 0.0)], axis=1
    ).astype(bf16)
    packed_grad = jnp.concatenate(
        [jnp.where(first_half, 0.0, turned(grad_own)), jnp.where(first_half, 0.0, grad_own)],
        axis=1,
    ).astype(bf16)
    key_values = jnp.concatenate([own[...], other[...]], axis=1)
    tokens = key_values.shape[0]
    scores = dot_nt(packed_query, key_values) * scale
    row = lax.broadcasted_iota(jnp.int32, (heads * rows, tokens), 0) % rows + place[1]
    causal = row >= lax.broadcasted_iota(jnp.int32, (heads * rows, tokens), 1)
    scores = jnp.where(causal, scores, -jnp.inf)
    shifted = jnp.exp(scores - jnp.max(scores, axis=1, keepdims=True))
    probs = shifted / jnp.sum(shifted, axis=1, keepdims=True)
    prob_weights = probs.astype(bf16)
    mixed = dot(prob_weights, key_values)
    attention = reordered(
        jnp.where(first_half, turned(mixed[:, :HEAD_DIM]), mixed[:, HEAD_DIM:])
    ).astype(bf16)
    delta = jnp.sum(grad * attention.astype(f32), axis=1, keepdims=True)
    prob_grad = dot_nt(packed_grad, key_values)
    score_grad = (probs * (prob_grad - delta) * scale).astype(bf16)
    mixed = dot(score_grad, key_values)
    query_grad = rope(
        reordered(jnp.where(first_half, mixed[:, :HEAD_DIM], turned(mixed[:, HEAD_DIM:]))), -1.0
    ).astype(bf16)
    key_value_grad = dot_tn(
        jnp.concatenate([score_grad, prob_weights], axis=0),
        jnp.concatenate([packed_query, packed_grad], axis=0),
    )
    kept[...] = key_value_grad[:, :HEAD_DIM]
    given[...] = key_value_grad[:, HEAD_DIM:].astype(bf16)
    low = joint[:, 2 * cols :]
    out_rank = low[:, 3 * ADAPTER_RANK : 4 * ADAPTER_RANK]
    for h in range(heads):
        lanes = slice(h * HEAD_DIM, (h + 1) * HEAD_DIM)
        of_head = attention[h * rows : (h + 1) * rows]
        riding[:, lanes] = query_grad[h * rows : (h + 1) * rows]
        attention_rows[:, lanes] = of_head
        riding[h * ADAPTER_RANK : (h + 1) * ADAPTER_RANK, cols : cols + HEAD_DIM] = dot_tn(
            out_rank, of_head
        ).astype(bf16)
    riding[:, cols + HEAD_DIM :] = low


def shards(
    hidden,
    upstream,
    query_frozen_weight,
    key_value_frozen_weight,
    output_frozen_weight,
    adapter_down,
    query_up_map,
    key_value_up_maps,
    output_down_map,
    output_up,
):
    ffn_count = lax.axis_size("ffn")
    width_count = lax.axis_size("width")
    ffn_index = lax.axis_index("ffn")
    width_index = lax.axis_index("width")
    parity = ffn_index % 2
    same_core = by_core(ffn_count)
    own_rows, width_cols = hidden.shape
    token_count = own_rows * ffn_count
    query_rows = token_count // width_count
    query_cols = query_frozen_weight.shape[1]
    key_cols = key_value_frozen_weight.shape[2]
    heads = query_cols // HEAD_DIM
    rank = ADAPTER_RANK
    score_scale = 1.0 / math.sqrt(HEAD_DIM)
    row_positions = width_index * query_rows + jnp.arange(query_rows, dtype=jnp.int32)

    query_weight = (
        query_frozen_weight.astype(f32) + adapter_scale * dot_tn(adapter_down[0], query_up_map)
    ).astype(bf16)
    key_value_weight = jnp.concatenate(
        [
            key_value_frozen_weight[k].astype(f32)
            + adapter_scale * dot_tn(adapter_down[k + 1], key_value_up_maps[k])
            for k in range(2)
        ],
        axis=1,
    ).astype(bf16)
    output_weight = (
        output_frozen_weight.astype(f32) + adapter_scale * dot_tn(output_down_map, output_up)
    ).astype(bf16)
    down = adapter_down.reshape(3 * rank, width_cols)
    low_weight = jnp.concatenate(
        [
            jnp.pad(down, ((0, HEAD_DIM - 3 * rank), (0, 0))),
            jnp.pad(output_up, ((3 * rank, HEAD_DIM - 4 * rank), (0, 0))),
        ],
        axis=1,
    ).T
    output_weight = output_weight.T
    query_tables = rope_tables(row_positions, 0, HEAD_DIM)
    key_tables = rope_tables(row_positions, ffn_index * key_cols, key_cols)
    input_weight = jnp.concatenate([query_weight, key_value_weight], axis=1).T
    input_weight, query_tables, key_tables = lax.optimization_barrier(
        (input_weight, query_tables, key_tables)
    )

    both = jnp.concatenate([hidden, upstream], axis=1)
    own_core = sent_to_all(both, "ffn", same_core)
    own_core, low_weight, output_weight, key_value_weight, query_weight = lax.optimization_barrier(
        (own_core, low_weight, output_weight, key_value_weight, query_weight)
    )
    other_core = from_partner(own_core)
    rows = jnp.where(
        parity == 0,
        jnp.stack([own_core, other_core], axis=1),
        jnp.stack([other_core, own_core], axis=1),
    ).reshape(token_count, 2 * width_cols)
    hidden_rows = rows[:, :width_cols]
    upstream_rows = rows[:, width_cols:]

    place = jnp.stack([parity, width_index * query_rows]).astype(jnp.int32)
    smem = pl.BlockSpec(memory_space=pltpu.SMEM)
    vmem = pl.BlockSpec(memory_space=pltpu.VMEM)
    weights = (query_weight, output_weight, low_weight, key_value_weight)

    def of_blocks(blocks):
        return (
            jax.ShapeDtypeStruct((blocks, own_rows, 2 * query_cols + HEAD_DIM), bf16),
            jax.ShapeDtypeStruct((blocks, own_rows, 2 * key_cols), bf16),
        )

    cost = pl.CostEstimate(
        flops=token_count * width_cols * (2 * query_cols + 2 * HEAD_DIM),
        bytes_accessed=2**22,
        transcendentals=0,
    )
    own_parts = pl.pallas_call(
        own_projections,
        out_shape=of_blocks(ffn_count // 2),
        in_specs=[vmem] * 5,
        out_specs=(vmem, vmem),
        cost_estimate=cost,
        compiler_params=pltpu.CompilerParams(vmem_limit_bytes=20 * 2**20),
        name="own_projections",
    )(own_core, *weights)
    joint_part, key_value_part = pl.pallas_call(
        all_projections,
        out_shape=of_blocks(ffn_count),
        in_specs=[smem] + [vmem] * 7,
        out_specs=(vmem, vmem),
        cost_estimate=cost,
        compiler_params=pltpu.CompilerParams(vmem_limit_bytes=20 * 2**20),
        name="all_projections",
    )(place, other_core, *weights, *own_parts)
    joint_part = joint_part.reshape(token_count, -1)
    key_value_part = key_value_part.reshape(token_count, -1)
    joint_rows = lax.psum_scatter(joint_part, "width", scatter_dimension=0, tiled=True)

    key_value_sum = pieces_summed(key_value_part, "width")
    key_value_rows = jnp.concatenate(
        [rotate(key_value_sum[:, :key_cols], key_tables, 1.0), key_value_sum[:, key_cols:]], axis=1
    ).astype(bf16)
    own_half = lax.all_gather(key_value_rows, "width", axis=0, tiled=True)
    other_half = from_partner(own_half)

    riding, attention_rows, kept, given = pl.pallas_call(
        functools.partial(attention_block, heads=heads, scale=score_scale),
        out_shape=(
            jax.ShapeDtypeStruct((query_rows, query_cols + 2 * HEAD_DIM), bf16),
            jax.ShapeDtypeStruct((query_rows, query_cols), bf16),
            jax.ShapeDtypeStruct((token_count, 2 * key_cols), f32),
            jax.ShapeDtypeStruct((token_count, 2 * key_cols), bf16),
        ),
        in_specs=[smem] + [vmem] * 5,
        out_specs=(vmem,) * 4,
        cost_estimate=pl.CostEstimate(
            flops=12 * heads * query_rows * token_count * HEAD_DIM,
            bytes_accessed=2**21,
            transcendentals=heads * query_rows * token_count,
        ),
        name="attention",
    )(place, joint_rows, own_half, other_half, *query_tables)
    query_grad = riding[:, :query_cols]

    gathered = lax.all_gather(riding, "width", axis=0, tiled=True)

    key_value_total = (kept + from_partner(given).astype(f32)).astype(bf16)
    terms = jnp.concatenate(
        [dot_nt(query_grad, query_up_map), dot_nt(attention_rows, output_down_map)], axis=1
    ).astype(bf16)
    key_value_total, terms = lax.optimization_barrier((key_value_total, terms))
    key_value_grad_sum = pieces_summed(key_value_total, "width")
    terms = lax.all_gather(terms, "ffn").astype(f32).sum(axis=0).astype(bf16)
    key_value_grad = jnp.concatenate(
        [
            rotate(key_value_grad_sum[:, :key_cols], key_tables, -1.0),
            key_value_grad_sum[:, key_cols:],
        ],
        axis=1,
    ).astype(bf16)
    key_value_gathered = lax.all_gather(
        jnp.concatenate([key_value_grad, terms], axis=1), "width", axis=0, tiled=True
    )
    key_value_grad_rows = key_value_gathered[:, : 2 * key_cols]
    key_value_terms = jnp.concatenate(
        [
            dot_nt(key_value_grad_rows[:, :key_cols], key_value_up_maps[0]),
            dot_nt(key_value_grad_rows[:, key_cols:], key_value_up_maps[1]),
        ],
        axis=1,
    ).astype(bf16)
    key_value_down = dot_tn(key_value_terms, hidden_rows)
    key_value_down = sent_to_all(key_value_down.astype(bf16), "ffn", same_core)

    given, kept = pl.pallas_call(
        input_parts,
        out_shape=(
            jax.ShapeDtypeStruct((token_count // 2, width_cols), bf16),
            jax.ShapeDtypeStruct((token_count // 2, width_cols), f32),
        ),
        in_specs=[smem] + [vmem] * 3,
        out_specs=(vmem, vmem),
        cost_estimate=pl.CostEstimate(
            flops=2 * token_count * width_cols * input_weight.shape[0],
            bytes_accessed=2**22,
            transcendentals=0,
        ),
        compiler_params=pltpu.CompilerParams(vmem_limit_bytes=20 * 2**20),
        name="input_parts",
    )(
        place,
        gathered.reshape(ffn_count, own_rows, -1),
        key_value_grad_rows.reshape(ffn_count, own_rows, -1),
        input_weight,
    )
    given = from_partner(given)
    given, key_value_down = lax.optimization_barrier((given, key_value_down))
    pair_sum = (kept + given.astype(f32)).astype(bf16)
    hidden_gradient = pieces_summed(pair_sum, "ffn", same_core).astype(bf16)
    key_value_down = key_value_down.astype(f32).sum(axis=0)
    key_value_down = key_value_down + from_partner(key_value_down)

    low = gathered[:, query_cols + HEAD_DIM :]
    query_rank = key_value_gathered[:, 2 * key_cols : 2 * key_cols + rank]
    outer_rank = key_value_gathered[:, 2 * key_cols + rank :]
    down_map_gradient = adapter_scale * jnp.concatenate(
        [dot_tn(query_rank, hidden_rows), key_value_down], axis=0
    ).reshape(adapter_down.shape)
    query_up_map_gradient = adapter_scale * dot_tn(low[:, :rank], gathered[:, :query_cols])
    key_value_up_maps_gradient = adapter_scale * jnp.stack(
        [
            dot_tn(low[:, rank : 2 * rank], key_value_grad_rows[:, :key_cols]),
            dot_tn(low[:, 2 * rank : 3 * rank], key_value_grad_rows[:, key_cols:]),
        ]
    )
    output_down_sum = (
        gathered[:, query_cols : query_cols + HEAD_DIM]
        .reshape(width_count, heads, rank, HEAD_DIM)
        .astype(f32)
        .sum(axis=0)
    )
    output_down_map_gradient = adapter_scale * output_down_sum.transpose(1, 0, 2).reshape(
        rank, query_cols
    )
    output_up_map_gradient = adapter_scale * dot_tn(outer_rank, upstream_rows)
    return (
        hidden_gradient,
        down_map_gradient,
        query_up_map_gradient,
        key_value_up_maps_gradient,
        output_down_map_gradient,
        output_up_map_gradient,
    )


def solution(mesh):
    placed = (
        P(("groups", "ffn"), "width"),
        P(("groups", "ffn"), "width"),
        P("width", "ffn"),
        P(None, "width", "ffn"),
        P("ffn", "width"),
        P("groups", None, "width"),
        P("groups", "ffn"),
        P("groups", None, "ffn"),
        P("groups", "ffn"),
        P("groups", "width"),
    )
    return jax.shard_map(
        shards,
        mesh=mesh,
        in_specs=placed,
        out_specs=(
            P(("groups", "ffn"), "width"),
            P("groups", None, "width"),
            P("groups", "ffn"),
            P("groups", None, "ffn"),
            P("groups", "ffn"),
            P("groups", "width"),
        ),
        check_vma=False,
    )
```

```python
import functools
import math

import jax
import jax.numpy as jnp
from jax import lax
from jax.experimental import pallas as pl
from jax.experimental.pallas import tpu as pltpu
from jax.sharding import PartitionSpec as P


HEAD_DIM = 128
ADAPTER_RANK = 16

adapter_scale = 2.0
rope_base = 500000.0

f32 = jnp.float32
bf16 = jnp.bfloat16


def dot(a, b):
    return jnp.dot(a, b, preferred_element_type=f32)


def dot_nt(a, b):
    return lax.dot_general(a, b, (((1,), (1,)), ((), ())), preferred_element_type=f32)


def dot_tn(a, b):
    return lax.dot_general(a, b, (((0,), (0,)), ((), ())), preferred_element_type=f32)


def by_core(size):
    return [[2 * k + c for k in range(size // 2)] for c in range(2)]


def exchanged(array, step):
    return lax.ppermute(array, "ffn", [(i, i ^ step) for i in range(lax.axis_size("ffn"))])


def from_partner(array):
    return exchanged(array, 1)


def sent_to_all(array, axis, groups=None):
    size = len(groups[0]) if groups else lax.axis_size(axis)
    copies = jnp.broadcast_to(array[None], (size, *array.shape))
    return lax.all_to_all(copies, axis, 0, 0, tiled=True, axis_index_groups=groups)


def pieces_summed(array, axis, groups=None):
    size = len(groups[0]) if groups else lax.axis_size(axis)
    pieces = array.reshape(size, array.shape[0] // size, *array.shape[1:])
    arrived = lax.all_to_all(pieces, axis, 0, 0, tiled=True, axis_index_groups=groups)
    return arrived.astype(f32).sum(axis=0)


def rope_tables(positions, first_dim, columns):
    dims = (first_dim + jnp.arange(columns, dtype=jnp.int32)) % HEAD_DIM
    pair_dims = dims - dims % 2
    frequency = jnp.exp(pair_dims.astype(f32) * (-math.log(rope_base) / HEAD_DIM))
    angles = positions.astype(f32)[:, None] * frequency[None, :]
    return jnp.cos(angles), jnp.sin(angles)


def rotate(values, tables, direction):
    cos, sin = tables
    is_even = jnp.arange(values.shape[-1], dtype=jnp.int32) % 2 == 0
    following = jnp.roll(values, -1, axis=-1)
    preceding = jnp.roll(values, 1, axis=-1)
    partner = jnp.where(is_even, -following, preceding)
    return values * cos + direction * partner * sin


def projected(part, query_weight, output_weight, low_weight, key_value_weight):
    chips, rows, both = part.shape
    tokens = part[...].reshape(chips * rows, both)
    hidden, upstream = tokens[:, : both // 2], tokens[:, both // 2 :]
    cols = query_weight.shape[1]
    end = cols + output_weight.shape[1]
    joint = (
        (dot(hidden, query_weight[...]).astype(bf16), slice(0, cols)),
        (dot(upstream, output_weight[...]).astype(bf16), slice(cols, end)),
        (dot(tokens, low_weight[...]).astype(bf16), slice(end, end + low_weight.shape[1])),
    )
    return joint, dot(hidden, key_value_weight[...]).astype(bf16)


def own_projections(
    own, query_weight, output_weight, low_weight, key_value_weight, joint, key_value
):
    values, of_key_value = projected(
        own, query_weight, output_weight, low_weight, key_value_weight
    )
    for value, lanes in values:
        joint[:, :, lanes] = value.reshape(*own.shape[:2], -1)
    key_value[...] = of_key_value.reshape(key_value.shape)


def all_projections(
    place,
    other,
    query_weight,
    output_weight,
    low_weight,
    key_value_weight,
    own_joint,
    own_key_value,
    joint,
    key_value,
):
    chips, rows, _ = other.shape
    values, of_key_value = projected(
        other, query_weight, output_weight, low_weight, key_value_weight
    )
    core = place[0]
    for chip in range(chips):
        here = slice(chip * rows, (chip + 1) * rows)
        joint[2 * chip + core] = own_joint[chip]
        key_value[2 * chip + core] = own_key_value[chip]
        for value, lanes in values:
            joint[2 * chip + 1 - core, :, lanes] = value[here]
        key_value[2 * chip + 1 - core] = of_key_value[here]


def input_parts(place, query_grad, key_value_grad, weight, given, kept):
    cols = weight.shape[0] - key_value_grad.shape[2]
    chips = query_grad.shape[0] // 2
    for out, core in ((given, 1 - place[0]), (kept, place[0])):
        blocks = [
            jnp.concatenate(
                [query_grad[2 * chip + core, :, :cols], key_value_grad[2 * chip + core]], axis=1
            )
            for chip in range(chips)
        ]
        out[...] = dot(jnp.concatenate(blocks, axis=0), weight[...]).astype(out.dtype)


def attention_block(
    place, joint, own, other, cos, sin, riding, attention_rows, kept, given, *, heads, scale
):
    swapped = place[0] == 1
    rows = joint.shape[0]
    cols = heads * HEAD_DIM
    half = HEAD_DIM // 2

    def stacked(start):
        return jnp.concatenate(
            [joint[:, start + h * HEAD_DIM : start + (h + 1) * HEAD_DIM] for h in range(heads)],
            axis=0,
        ).astype(f32)

    def turned(values):
        return pltpu.roll(values, half, 1)

    def reordered(values):
        return jnp.where(swapped, turned(values), values)

    lane = lax.broadcasted_iota(jnp.int32, (heads * rows, HEAD_DIM), 1)
    first_half = lane < half
    is_even = lane % 2 == 0
    cosines = jnp.concatenate([cos[...]] * heads, axis=0)
    sines = jnp.concatenate([sin[...]] * heads, axis=0)

    def rope(values, direction):
        partner = jnp.where(
            is_even, -pltpu.roll(values, HEAD_DIM - 1, 1), pltpu.roll(values, 1, 1)
        )
        return values * cosines + direction * partner * sines

    query = reordered(rope(stacked(0), 1.0).astype(bf16).astype(f32))
    grad = stacked(cols)
    grad_own = reordered(grad)
    packed_query = jnp.concatenate(
        [jnp.where(first_half, query, 0.0), jnp.where(first_half, turned(query), 0.0)], axis=1
    ).astype(bf16)
    packed_grad = jnp.concatenate(
        [jnp.where(first_half, 0.0, turned(grad_own)), jnp.where(first_half, 0.0, grad_own)],
        axis=1,
    ).astype(bf16)
    key_values = jnp.concatenate([own[...], other[...]], axis=1)
    tokens = key_values.shape[0]
    scores = dot_nt(packed_query, key_values) * scale
    row = lax.broadcasted_iota(jnp.int32, (heads * rows, tokens), 0) % rows + place[1]
    causal = row >= lax.broadcasted_iota(jnp.int32, (heads * rows, tokens), 1)
    scores = jnp.where(causal, scores, -jnp.inf)
    shifted = jnp.exp(scores - jnp.max(scores, axis=1, keepdims=True))
    probs = shifted / jnp.sum(shifted, axis=1, keepdims=True)
    prob_weights = probs.astype(bf16)
    mixed = dot(prob_weights, key_values)
    attention = reordered(
        jnp.where(first_half, turned(mixed[:, :HEAD_DIM]), mixed[:, HEAD_DIM:])
    ).astype(bf16)
    delta = jnp.sum(grad * attention.astype(f32), axis=1, keepdims=True)
    prob_grad = dot_nt(packed_grad, key_values)
    score_grad = (probs * (prob_grad - delta) * scale).astype(bf16)
    mixed = dot(score_grad, key_values)
    query_grad = rope(
        reordered(jnp.where(first_half, mixed[:, :HEAD_DIM], turned(mixed[:, HEAD_DIM:]))), -1.0
    ).astype(bf16)
    key_value_grad = dot_tn(
        jnp.concatenate([score_grad, prob_weights], axis=0),
        jnp.concatenate([packed_query, packed_grad], axis=0),
    )
    kept[...] = key_value_grad[:, :HEAD_DIM]
    given[...] = key_value_grad[:, HEAD_DIM:].astype(bf16)
    low = joint[:, 2 * cols :]
    out_rank = low[:, 3 * ADAPTER_RANK : 4 * ADAPTER_RANK]
    for h in range(heads):
        lanes = slice(h * HEAD_DIM, (h + 1) * HEAD_DIM)
        of_head = attention[h * rows : (h + 1) * rows]
        riding[:, lanes] = query_grad[h * rows : (h + 1) * rows]
        attention_rows[:, lanes] = of_head
        riding[h * ADAPTER_RANK : (h + 1) * ADAPTER_RANK, cols : cols + HEAD_DIM] = dot_tn(
            out_rank, of_head
        ).astype(bf16)
    riding[:, cols + HEAD_DIM :] = low


def shards(
    hidden,
    upstream,
    query_frozen_weight,
    key_value_frozen_weight,
    output_frozen_weight,
    adapter_down,
    query_up_map,
    key_value_up_maps,
    output_down_map,
    output_up,
):
    ffn_count = lax.axis_size("ffn")
    width_count = lax.axis_size("width")
    ffn_index = lax.axis_index("ffn")
    width_index = lax.axis_index("width")
    parity = ffn_index % 2
    same_core = by_core(ffn_count)
    own_rows, width_cols = hidden.shape
    token_count = own_rows * ffn_count
    query_rows = token_count // width_count
    query_cols = query_frozen_weight.shape[1]
    key_cols = key_value_frozen_weight.shape[2]
    heads = query_cols // HEAD_DIM
    rank = ADAPTER_RANK
    score_scale = 1.0 / math.sqrt(HEAD_DIM)
    row_positions = width_index * query_rows + jnp.arange(query_rows, dtype=jnp.int32)

    query_weight = (
        query_frozen_weight.astype(f32) + adapter_scale * dot_tn(adapter_down[0], query_up_map)
    ).astype(bf16)
    key_value_weight = jnp.concatenate(
        [
            key_value_frozen_weight[k].astype(f32)
            + adapter_scale * dot_tn(adapter_down[k + 1], key_value_up_maps[k])
            for k in range(2)
        ],
        axis=1,
    ).astype(bf16)
    output_weight = (
        output_frozen_weight.astype(f32) + adapter_scale * dot_tn(output_down_map, output_up)
    ).astype(bf16)
    down = adapter_down.reshape(3 * rank, width_cols)
    low_weight = jnp.concatenate(
        [
            jnp.pad(down, ((0, HEAD_DIM - 3 * rank), (0, 0))),
            jnp.pad(output_up, ((3 * rank, HEAD_DIM - 4 * rank), (0, 0))),
        ],
        axis=1,
    ).T
    output_weight = output_weight.T
    query_tables = rope_tables(row_positions, 0, HEAD_DIM)
    key_tables = rope_tables(row_positions, ffn_index * key_cols, key_cols)
    input_weight = jnp.concatenate([query_weight, key_value_weight], axis=1).T
    input_weight, query_tables, key_tables = lax.optimization_barrier(
        (input_weight, query_tables, key_tables)
    )

    both = jnp.concatenate([hidden, upstream], axis=1)
    own_core = sent_to_all(both, "ffn", same_core)
    own_core, low_weight, output_weight, key_value_weight, query_weight = lax.optimization_barrier(
        (own_core, low_weight, output_weight, key_value_weight, query_weight)
    )
    other_core = from_partner(own_core)
    rows = jnp.where(
        parity == 0,
        jnp.stack([own_core, other_core], axis=1),
        jnp.stack([other_core, own_core], axis=1),
    ).reshape(token_count, 2 * width_cols)
    hidden_rows = rows[:, :width_cols]
    upstream_rows = rows[:, width_cols:]

    place = jnp.stack([parity, width_index * query_rows]).astype(jnp.int32)
    smem = pl.BlockSpec(memory_space=pltpu.SMEM)
    vmem = pl.BlockSpec(memory_space=pltpu.VMEM)
    weights = (query_weight, output_weight, low_weight, key_value_weight)

    def of_blocks(blocks):
        return (
            jax.ShapeDtypeStruct((blocks, own_rows, 2 * query_cols + HEAD_DIM), bf16),
            jax.ShapeDtypeStruct((blocks, own_rows, 2 * key_cols), bf16),
        )

    cost = pl.CostEstimate(
        flops=token_count * width_cols * (2 * query_cols + 2 * HEAD_DIM),
        bytes_accessed=2**22,
        transcendentals=0,
    )
    own_parts = pl.pallas_call(
        own_projections,
        out_shape=of_blocks(ffn_count // 2),
        in_specs=[vmem] * 5,
        out_specs=(vmem, vmem),
        cost_estimate=cost,
        compiler_params=pltpu.CompilerParams(vmem_limit_bytes=20 * 2**20),
        name="own_projections",
    )(own_core, *weights)
    joint_part, key_value_part = pl.pallas_call(
        all_projections,
        out_shape=of_blocks(ffn_count),
        in_specs=[smem] + [vmem] * 7,
        out_specs=(vmem, vmem),
        cost_estimate=cost,
        compiler_params=pltpu.CompilerParams(vmem_limit_bytes=20 * 2**20),
        name="all_projections",
    )(place, other_core, *weights, *own_parts)
    joint_part = joint_part.reshape(token_count, -1)
    key_value_part = key_value_part.reshape(token_count, -1)
    joint_rows = lax.psum_scatter(joint_part, "width", scatter_dimension=0, tiled=True)

    key_value_sum = pieces_summed(key_value_part, "width")
    key_value_rows = jnp.concatenate(
        [rotate(key_value_sum[:, :key_cols], key_tables, 1.0), key_value_sum[:, key_cols:]], axis=1
    ).astype(bf16)
    own_half = lax.all_gather(key_value_rows, "width", axis=0, tiled=True)
    other_half = from_partner(own_half)

    riding, attention_rows, kept, given = pl.pallas_call(
        functools.partial(attention_block, heads=heads, scale=score_scale),
        out_shape=(
            jax.ShapeDtypeStruct((query_rows, query_cols + 2 * HEAD_DIM), bf16),
            jax.ShapeDtypeStruct((query_rows, query_cols), bf16),
            jax.ShapeDtypeStruct((token_count, 2 * key_cols), f32),
            jax.ShapeDtypeStruct((token_count, 2 * key_cols), bf16),
        ),
        in_specs=[smem] + [vmem] * 5,
        out_specs=(vmem,) * 4,
        cost_estimate=pl.CostEstimate(
            flops=12 * heads * query_rows * token_count * HEAD_DIM,
            bytes_accessed=2**21,
            transcendentals=heads * query_rows * token_count,
        ),
        name="attention",
    )(place, joint_rows, own_half, other_half, *query_tables)
    query_grad = riding[:, :query_cols]

    gathered = lax.all_gather(riding, "width", axis=0, tiled=True)

    key_value_total = (kept + from_partner(given).astype(f32)).astype(bf16)
    terms = jnp.concatenate(
        [dot_nt(query_grad, query_up_map), dot_nt(attention_rows, output_down_map)], axis=1
    ).astype(bf16)
    key_value_total, terms = lax.optimization_barrier((key_value_total, terms))
    key_value_grad_sum = pieces_summed(key_value_total, "width")
    terms = lax.all_gather(terms, "ffn").astype(f32).sum(axis=0).astype(bf16)
    key_value_grad = jnp.concatenate(
        [
            rotate(key_value_grad_sum[:, :key_cols], key_tables, -1.0),
            key_value_grad_sum[:, key_cols:],
        ],
        axis=1,
    ).astype(bf16)
    key_value_gathered = lax.all_gather(
        jnp.concatenate([key_value_grad, terms], axis=1), "width", axis=0, tiled=True
    )
    key_value_grad_rows = key_value_gathered[:, : 2 * key_cols]
    key_value_terms = jnp.concatenate(
        [
            dot_nt(key_value_grad_rows[:, :key_cols], key_value_up_maps[0]),
            dot_nt(key_value_grad_rows[:, key_cols:], key_value_up_maps[1]),
        ],
        axis=1,
    ).astype(bf16)
    key_value_down = dot_tn(key_value_terms, hidden_rows)
    key_value_down = sent_to_all(key_value_down.astype(bf16), "ffn", same_core)

    given, kept = pl.pallas_call(
        input_parts,
        out_shape=(
            jax.ShapeDtypeStruct((token_count // 2, width_cols), bf16),
            jax.ShapeDtypeStruct((token_count // 2, width_cols), f32),
        ),
        in_specs=[smem] + [vmem] * 3,
        out_specs=(vmem, vmem),
        cost_estimate=pl.CostEstimate(
            flops=2 * token_count * width_cols * input_weight.shape[0],
            bytes_accessed=2**22,
            transcendentals=0,
        ),
        compiler_params=pltpu.CompilerParams(vmem_limit_bytes=20 * 2**20),
        name="input_parts",
    )(
        place,
        gathered.reshape(ffn_count, own_rows, -1),
        key_value_grad_rows.reshape(ffn_count, own_rows, -1),
        input_weight,
    )
    given = from_partner(given)
    outer_rank = key_value_gathered[:, 2 * key_cols + rank :]
    given, key_value_down, outer_rank = lax.optimization_barrier(
        (given, key_value_down, outer_rank)
    )
    pair_sum = (kept + given.astype(f32)).astype(bf16)
    hidden_gradient = pieces_summed(pair_sum, "ffn", same_core).astype(bf16)
    key_value_down = key_value_down.astype(f32).sum(axis=0)
    key_value_down = key_value_down + from_partner(key_value_down)

    low = gathered[:, query_cols + HEAD_DIM :]
    query_rank = key_value_gathered[:, 2 * key_cols : 2 * key_cols + rank]
    down_map_gradient = adapter_scale * jnp.concatenate(
        [dot_tn(query_rank, hidden_rows), key_value_down], axis=0
    ).reshape(adapter_down.shape)
    query_up_map_gradient = adapter_scale * dot_tn(low[:, :rank], gathered[:, :query_cols])
    key_value_up_maps_gradient = adapter_scale * jnp.stack(
        [
            dot_tn(low[:, rank : 2 * rank], key_value_grad_rows[:, :key_cols]),
            dot_tn(low[:, 2 * rank : 3 * rank], key_value_grad_rows[:, key_cols:]),
        ]
    )
    output_down_sum = (
        gathered[:, query_cols : query_cols + HEAD_DIM]
        .reshape(width_count, heads, rank, HEAD_DIM)
        .astype(f32)
        .sum(axis=0)
    )
    output_down_map_gradient = adapter_scale * output_down_sum.transpose(1, 0, 2).reshape(
        rank, query_cols
    )
    output_up_map_gradient = adapter_scale * dot_tn(outer_rank, upstream_rows)
    return (
        hidden_gradient,
        down_map_gradient,
        query_up_map_gradient,
        key_value_up_maps_gradient,
        output_down_map_gradient,
        output_up_map_gradient,
    )


def solution(mesh):
    placed = (
        P(("groups", "ffn"), "width"),
        P(("groups", "ffn"), "width"),
        P("width", "ffn"),
        P(None, "width", "ffn"),
        P("ffn", "width"),
        P("groups", None, "width"),
        P("groups", "ffn"),
        P("groups", None, "ffn"),
        P("groups", "ffn"),
        P("groups", "width"),
    )
    return jax.shard_map(
        shards,
        mesh=mesh,
        in_specs=placed,
        out_specs=(
            P(("groups", "ffn"), "width"),
            P("groups", None, "width"),
            P("groups", "ffn"),
            P("groups", None, "ffn"),
            P("groups", "ffn"),
            P("groups", "width"),
        ),
        check_vma=False,
    )
```
